512 devices in a mesh: groups: 2 (over y), sky: 32 (over z), epoch: 4 (over x), band: 2 (over core).
Axes of the slice: x: 4, y: 2, z: 32, core: 2. Of those that a mesh axis runs over, the one named last changes fastest.
The devices are a block of a 4x8x32 slice.
Arguments:
- slot_pixels: bfloat16 [12288, 6, 32, 512], P(('groups', 'sky', 'epoch'), 'band'), parts along dimension 0, may hold values from -6 to 6
- slot_tile: int32 [12288, 1], P(('groups', 'sky', 'epoch')), parts along dimension 0, may hold values from 0 to 31; in each aligned block of 48 rows (0 to 47, 48 to 95, ...) at most 2 rows name the same one
- slot_offset: int32 [12288, 2], P(('groups', 'sky', 'epoch')), parts along dimension 0, may hold values from -5 to 5
- slot_frac: bfloat16 [12288, 2], P(('groups', 'sky', 'epoch')), parts along dimension 0, may hold values from 0.049804688 to 0.94921875
- slot_sigma: bfloat16 [12288, 6], P(('groups', 'sky', 'epoch'), 'band'), parts along dimension 0, may hold values from 0.5 to 2
- clip_mask: int32 [12288, 6, 16], P(('groups', 'sky', 'epoch')), parts along dimension 0, may hold values 0 or 1
- slot_count: int32 [256], P(('groups', 'sky', 'epoch')), parts along dimension 0, may hold values from 36 to 48
- template: bfloat16 [6, 2048, 512], P('band', ('groups', 'sky')), parts along dimension 1, may hold values from -6 to 6
- prior_weight: float32 [6, 2048], P('band', ('groups', 'sky')), parts along dimension 1, may hold values from 0.5 to 4
Outputs:
- coadd_image: bfloat16 [6, 2048, 512], P('band', ('groups', 'sky'), 'epoch'), parts along dimension 1
- depth_norm: bfloat16 [6, 2048, 512], P('band', ('groups', 'sky'), 'epoch'), parts along dimension 1
The draws below stay inside these ranges and needn't reach their ends.
There are 2 independent parts, one for each index of `groups`. The reference program is written for one: setup_inputs(seed, part) draws one part's arguments, and reference() takes and returns one part's arrays. A program takes and returns all parts, laid end to end along the dimension named above; each array names one. Nothing has to cross between parts.
Inputs may be any that keep to these rules, and one draw needn't show every extreme that they name: `slot_tile`: among the 48 rows of one reading device no owner is named more than 2 times, a bound that some block reaches. `slot_count`: slots of a reading device at or after its count are padding.
All inputs are finite; a program needn't handle non-finite values. No bound on the sum of `clip_mask` on one device may be relied on, other than what follows from the above.
Results may differ from the reference program's by a relative error of at most 0.014.
Values may be sent and summed in bfloat16 or wider, within the bound.
No kernel may reach another device: no remote copies, remote signals or barrier semaphores. Data moves between devices by JAX's collectives and lax.ppermute only.
A program may use at most 64 MiB of HBM per device.

```python
import math
import jax
import jax.numpy as jnp
import numpy as np
from jax import lax

BAND_COUNT = 6
TILE_COLS = 512
ROWS_DEV = 32
MAX_SHIFT = 5
MARGIN = 8
CAPACITY = 2
SLOT_DEV = 48
SLOT_TOTAL = 6144
PATCH_ROWS = 1024
N_SKY = 32
N_EPOCH = 4


def plant(array, key, least, high):
    longest = array.shape.index(max(array.shape))
    spots = []
    for shift in (0, 1):
        where = [jax.random.randint(jax.random.fold_in(key, axis), (), 0, length) for axis, length in enumerate(array.shape)]
        where[longest] = (where[longest] + shift) % array.shape[longest]
        spots.append(tuple(where))
    return array.at[spots[0]].set(least).at[spots[1]].set(high)


def block_levels(own_key, extent, shards, smallest, high):
    level = 1.0
    for position, parts in shards:
        steps = jax.random.uniform(jax.random.fold_in(jax.random.fold_in(own_key, 6), position), (parts,), jnp.float32, smallest / len(shards), high / len(shards))
        level = level * jnp.repeat(jnp.exp(steps), extent[position] // parts).reshape((-1,) + (1,) * (len(extent) - 1 - position))
    return level


def shared_out(stream_key, own, number, rows, amount, top, most, skew):
    sequence = jax.random.permutation(stream_key, amount)
    heavy_load, usual = portions_of(amount, rows * top, most, skew, True), portions_of(amount, rows * top, most, skew, False)
    places = jnp.arange(amount)

    def named(lengths, offset_by):
        used = int((lengths > 0).sum())
        fixed = max(1, used // 4)
        moved = fixed + (places - fixed + offset_by * (used - fixed)) % max(1, amount - fixed)
        return jnp.zeros((amount,), jnp.int32).at[sequence[jnp.where(places < fixed, places, moved)]].set(jnp.asarray(lengths, jnp.int32))

    lengths = jnp.where(number % 4 == 0, named(heavy_load, number // 4), named(usual, number - number // 4 - 1))
    mixed = jax.random.permutation(jax.random.fold_in(own, 3), amount)
    giver, receiver = mixed[0:amount // 2 * 2:2], mixed[1:amount // 2 * 2:2]
    slack = jnp.minimum(lengths[giver] - 1, most - lengths[receiver]) // 2
    slack = jnp.where((giver == sequence[0]) | (receiver == sequence[0]) | (lengths[receiver] == 0), 0, jnp.maximum(slack, 0))
    moved = jax.random.randint(jax.random.fold_in(own, 4), (amount // 2,), 0, 1 << 20) % (slack + 1)
    lengths = lengths.at[giver].add(-moved).at[receiver].add(moved)
    labels = jnp.searchsorted(jnp.cumsum(lengths), jnp.arange(rows * top), side="right").astype(jnp.int32)
    table = labels.reshape(top, rows).T
    table = table[jax.random.permutation(jax.random.fold_in(own, 1), rows)]
    offset_by = jax.random.randint(jax.random.fold_in(own, 2), (rows, 1), 0, top)
    return jnp.take_along_axis(table, (jnp.arange(top)[None, :] + offset_by) % top, axis=1)


def portions_of(amount, total, reach, lean, full):
    loads = [(1 << 20) // math.isqrt(standing ** lean) + 1 for standing in range(1, amount + 1)]
    largest = reach if full else min(reach, max(-(-total // amount), total * loads[0] // sum(loads)))
    least = 1 if total - largest >= amount - 1 else 0
    counts, spare = [largest] + [least] * (amount - 1), total - largest - least * (amount - 1)
    while spare > 0:
        movable = [i for i in range(1, amount) if counts[i] < largest] or [i for i in range(1, amount) if counts[i] < reach]
        pool, left = sum([loads[i] for i in movable]), spare
        for i in movable:
            more = min(reach - counts[i], max(1, left * loads[i] // pool), spare)
            counts[i] = counts[i] + more
            spare = spare - more
    return np.array(counts)


def gaussian(rng, dims, spread, most, cuts=(), kind=jnp.bfloat16):
    result = spread * jax.random.normal(rng, dims, jnp.float32)
    if cuts:
        result = result * block_levels(rng, dims, cuts, -0.22, 0.18)
    return jnp.clip(result, -most, most).astype(kind)


def setup_inputs(seed: int = 0, part: int = 0) -> dict:
    splits = jax.random.split(jax.random.key(seed), 10)
    part_splits = jax.random.split(jax.random.fold_in(splits[9], part), 10)
    slot_pixels = gaussian(part_splits[0], (SLOT_TOTAL, BAND_COUNT, ROWS_DEV, TILE_COLS), 1.0, 6.0, ((0, 128), (1, 2)))
    slot_tile_keys = jax.random.split(jax.random.fold_in(part_splits[1], 1), SLOT_TOTAL // SLOT_DEV)
    slot_tile_turns = jax.random.permutation(jax.random.fold_in(part_splits[1], 3), SLOT_TOTAL // SLOT_DEV)
    slot_tile = jax.vmap(lambda own, number: shared_out(jax.random.fold_in(part_splits[1], 2), own, number, SLOT_DEV, N_SKY, 1, CAPACITY, 2))(slot_tile_keys, slot_tile_turns).reshape((SLOT_TOTAL, 1))
    slot_offset = plant(jax.random.randint(part_splits[2], (SLOT_TOTAL, 2), 0 - MAX_SHIFT, MAX_SHIFT + 1), jax.random.fold_in(part_splits[2], 1), 0 - MAX_SHIFT, MAX_SHIFT).astype(jnp.int32)
    slot_frac = jnp.clip(0.049804688 + 0.89941406 * jax.random.uniform(part_splits[3], (SLOT_TOTAL, 2), jnp.float32) ** block_levels(part_splits[3], (SLOT_TOTAL, 2), ((0, 128),), -0.2, 0.2), 0.049804688, 0.94921875).astype(jnp.bfloat16)
    slot_sigma = jnp.clip(jnp.exp(math.log(2.0) - 1.3862944 * jax.random.uniform(part_splits[4], (SLOT_TOTAL, BAND_COUNT), jnp.float32) ** block_levels(part_splits[4], (SLOT_TOTAL, BAND_COUNT), ((0, 128), (1, 2)), -0.2, 0.2)), 0.5, 2.0).astype(jnp.bfloat16)
    clip_mask = plant((jax.random.randint(part_splits[5], (SLOT_TOTAL, (ROWS_DEV + 2 * MARGIN) // 8, TILE_COLS // 32), 0, 8) < 7).astype(jnp.int32), jax.random.fold_in(part_splits[5], 1), 0, 1)
    slot_count = plant(jax.random.randint(part_splits[6], (N_SKY * N_EPOCH,), 3 * SLOT_DEV // 4, SLOT_DEV + 1), jax.random.fold_in(part_splits[6], 1), 3 * SLOT_DEV // 4, SLOT_DEV).astype(jnp.int32)
    template = gaussian(part_splits[7], (BAND_COUNT, PATCH_ROWS, TILE_COLS), 1.0, 6.0, ((0, 2), (1, 32)))
    prior_weight = jnp.clip(jnp.exp(math.log(4.0) - 2.0794415 * jax.random.uniform(part_splits[8], (BAND_COUNT, PATCH_ROWS), jnp.float32) ** block_levels(part_splits[8], (BAND_COUNT, PATCH_ROWS), ((0, 2), (1, 32)), -0.2, 0.2)), 0.5, 4.0)
    return {"slot_pixels": slot_pixels, "slot_tile": slot_tile, "slot_offset": slot_offset, "slot_frac": slot_frac, "slot_sigma": slot_sigma, "clip_mask": clip_mask, "slot_count": slot_count, "template": template, "prior_weight": prior_weight}


CLIP_WIDTH = 3.0


def lanczos(distance):
    inside = jnp.abs(distance) < 3.0
    return jnp.where(inside, jnp.sinc(distance) * jnp.sinc(distance / 3.0), 0.0)


def tap_weights(fraction):
    steps_back = jnp.arange(-3, 3, dtype=jnp.int32)
    distance = (-steps_back).astype(jnp.float32) - fraction
    rounded = lanczos(distance).astype(jnp.bfloat16)
    return lax.optimization_barrier(rounded).astype(jnp.float32)


def reference(slot_pixels, slot_tile, slot_offset, slot_frac, slot_sigma, clip_mask, slot_count, template, prior_weight):
    slot_number = slot_pixels.shape[0]
    canvas_rows = ROWS_DEV + 2 * MARGIN
    patch_rows = template.shape[1]
    tile_cols = template.shape[2]
    template_pad = jnp.pad(template.astype(jnp.float32), ((0, 0), (MARGIN, MARGIN), (0, 0)))
    empty_sums = jnp.zeros((BAND_COUNT, patch_rows + 2 * MARGIN, tile_cols), jnp.float32)
    row_index = jnp.arange(canvas_rows, dtype=jnp.int32)
    col_index = jnp.arange(tile_cols, dtype=jnp.int32)

    def one_slot(carried, slot_index):
        flux_sums, weight_sums = carried
        pixels = lax.dynamic_index_in_dim(slot_pixels, slot_index, 0, keepdims=False).astype(jnp.float32)
        tile_index = slot_tile[slot_index, 0]
        shift_y = slot_offset[slot_index, 0]
        shift_x = slot_offset[slot_index, 1]
        taps_y = tap_weights(slot_frac[slot_index, 0].astype(jnp.float32))
        taps_x = tap_weights(slot_frac[slot_index, 1].astype(jnp.float32))
        is_live = ((slot_index % SLOT_DEV) < slot_count[slot_index // SLOT_DEV]).astype(jnp.float32)
        padded = jnp.pad(pixels, ((0, 0), (0, 0), (MARGIN, MARGIN)))
        columns = jnp.zeros((BAND_COUNT, ROWS_DEV, tile_cols), jnp.float32)
        col_cover = jnp.zeros((tile_cols,), jnp.float32)
        for tap_index in range(6):
            step_back = tap_index - 3
            shifted = lax.dynamic_slice_in_dim(padded, MARGIN - shift_x + step_back, tile_cols, 2)
            columns = columns + taps_x[tap_index] * shifted
            source_col = col_index - shift_x + step_back
            inside = (source_col >= 0) & (source_col < tile_cols)
            col_cover = col_cover + jnp.where(inside, taps_x[tap_index], 0.0)
        columns = lax.optimization_barrier(columns.astype(jnp.bfloat16)).astype(jnp.float32)
        column_pad = jnp.pad(columns, ((0, 0), (2 * MARGIN, 2 * MARGIN), (0, 0)))
        warped = jnp.zeros((BAND_COUNT, canvas_rows, tile_cols), jnp.float32)
        row_cover = jnp.zeros((canvas_rows,), jnp.float32)
        for tap_index in range(6):
            step_back = tap_index - 3
            shifted = lax.dynamic_slice_in_dim(column_pad, MARGIN - shift_y + step_back, canvas_rows, 1)
            warped = warped + taps_y[tap_index] * shifted
            source_row = row_index - MARGIN - shift_y + step_back
            inside = (source_row >= 0) & (source_row < ROWS_DEV)
            row_cover = row_cover + jnp.where(inside, taps_y[tap_index], 0.0)
        row_cover = jnp.clip(row_cover, 0.0, 1.0)
        col_cover = jnp.clip(col_cover, 0.0, 1.0)
        block_mask = clip_mask[slot_index].astype(jnp.float32)
        expanded = jnp.repeat(jnp.repeat(block_mask, 8, axis=0), 32, axis=1) * is_live
        plane = (expanded * row_cover[:, None]) * col_cover[None, :]
        sigmas = slot_sigma[slot_index].astype(jnp.float32)
        weight = plane[None] / (sigmas * sigmas)[:, None, None]
        framed = lax.dynamic_slice_in_dim(template_pad, tile_index * ROWS_DEV, canvas_rows, 1)
        scale = CLIP_WIDTH * sigmas[:, None, None]
        clipped = framed + scale * jnp.tanh((warped - framed) / scale)
        start = tile_index * ROWS_DEV
        old_flux = lax.dynamic_slice_in_dim(flux_sums, start, canvas_rows, 1)
        old_weight = lax.dynamic_slice_in_dim(weight_sums, start, canvas_rows, 1)
        flux_sums = lax.dynamic_update_slice_in_dim(flux_sums, old_flux + weight * clipped, start, 1)
        weight_sums = lax.dynamic_update_slice_in_dim(weight_sums, old_weight + weight, start, 1)
        return (flux_sums, weight_sums), None

    (flux_sums, weight_sums), _ = lax.scan(one_slot, (empty_sums, empty_sums), jnp.arange(slot_number, dtype=jnp.int32))
    flux_sum = flux_sums[:, MARGIN:MARGIN + patch_rows]
    weight_sum = weight_sums[:, MARGIN:MARGIN + patch_rows]
    prior = prior_weight[:, :, None]
    coadd_image = ((flux_sum + prior * template.astype(jnp.float32)) / (weight_sum + prior)).astype(jnp.bfloat16)
    depth_map = weight_sum + prior
    band_mean = jnp.sum(depth_map, axis=(1, 2)) / (patch_rows * tile_cols)
    depth_norm = (depth_map / band_mean[:, None, None]).astype(jnp.bfloat16)
    return coadd_image, depth_norm
```

```python
import functools

import jax
import jax.numpy as jnp
from jax import lax
from jax.experimental import pallas as pl
from jax.experimental.pallas import tpu as pltpu
from jax.sharding import PartitionSpec as P

MARGIN = 8
CAPACITY = 2
CLIP_WIDTH = 3.0
TAPS = 6
ROW_BLOCK = 8
LANES = 128
GROUP = 8


def lanczos(distance):
    inside = jnp.abs(distance) < 3.0
    return jnp.where(inside, jnp.sinc(distance) * jnp.sinc(distance / 3.0), 0.0)


def tap_weights(fractions):
    gaps = 3.0 - jnp.arange(TAPS, dtype=jnp.float32)
    rounded = lanczos(gaps - fractions[..., None]).astype(jnp.bfloat16)
    return lax.optimization_barrier(rounded).astype(jnp.float32)


def cover(shifts, taps, index, length_in):
    total = jnp.zeros((shifts.shape[0], index.shape[0]), jnp.float32)
    for tap in range(TAPS):
        source = index[None, :] - shifts[:, None] + (tap - 3)
        inside = (source >= 0) & (source < length_in)
        total = total + jnp.where(inside, taps[:, tap][:, None], 0.0)
    return jnp.clip(total, 0.0, 1.0)


def column_kernel(ints, floats, pixels, out, tables):
    step = pl.program_id(0)
    slots, bands, rows, cols = pixels.shape
    blocks = cols // LANES
    edge = 16

    @pl.when(step == 0)
    def _():
        tables[...] = jnp.zeros_like(tables)

    def gap_base(first_row, count, offset):
        k = lax.broadcasted_iota(jnp.int32, (count, LANES), 0) + first_row
        j = lax.broadcasted_iota(jnp.int32, (count, LANES), 1)
        return j - k + offset

    def one(slot, table):
        at = step * slots + slot
        shift = ints[at]
        weights = [floats[at * TAPS + tap] for tap in range(TAPS)]

        def band_of(base):
            gap = base - shift
            value = jnp.zeros(base.shape, jnp.float32)
            for tap in range(TAPS):
                value = jnp.where(gap == 3 - tap, weights[tap], value)
            return value.astype(jnp.bfloat16)

        diagonal = band_of(gap_base(0, LANES, 0))
        upper = band_of(gap_base(LANES - edge, edge, LANES))
        lower = band_of(gap_base(0, edge, -LANES))
        for block in range(blocks):
            low, high = block * LANES, (block + 1) * LANES
            table[low:high, low:high] = diagonal
            if block + 1 < blocks:
                table[high - edge : high, high : high + LANES] = upper
                table[high : high + edge, low:high] = lower
        source = pixels[slot].reshape(bands * rows, cols)
        warped = jnp.dot(source, table[...], preferred_element_type=jnp.float32)
        out[slot] = warped.astype(out.dtype).reshape(bands, rows, cols)

    def pair(index, carry):
        for half in range(2):
            one(index * 2 + half, tables.at[half])
        return carry

    lax.fori_loop(0, slots // 2, pair, 0)


def warp_columns(pixels, shifts, taps):
    held, bands, rows, cols = pixels.shape
    return pl.pallas_call(
        column_kernel,
        grid=(held // GROUP,),
        out_shape=jax.ShapeDtypeStruct(pixels.shape, jnp.bfloat16),
        in_specs=[
            pl.BlockSpec(memory_space=pltpu.SMEM),
            pl.BlockSpec(memory_space=pltpu.SMEM),
            pl.BlockSpec((GROUP, bands, rows, cols), lambda g: (g, 0, 0, 0)),
        ],
        out_specs=pl.BlockSpec((GROUP, bands, rows, cols), lambda g: (g, 0, 0, 0)),
        scratch_shapes=[pltpu.VMEM((2, cols, cols), jnp.bfloat16)],
        compiler_params=pltpu.CompilerParams(dimension_semantics=("arbitrary",)),
        cost_estimate=pl.CostEstimate(
            flops=2 * held * bands * rows * cols * cols,
            bytes_accessed=4 * held * bands * rows * cols,
            transcendentals=0,
        ),
        name="columns",
    )(shifts, taps.reshape(-1), pixels)


def clip_kernel(ints, floats, columns, tables, row_cover, plane, template, out, framed, sums):
    step = pl.program_id(0)
    slots, bands, rows, cols = columns.shape
    owners = template.shape[0]
    canvas_rows = row_cover.shape[1]
    quarters = out.shape[0]
    width = cols // quarters

    @pl.when(step == 0)
    def _():
        ends = framed.shape[1]
        for band in range(bands):
            framed[band, 0:MARGIN, :] = jnp.zeros((MARGIN, cols), jnp.float32)
            framed[band, ends - MARGIN : ends, :] = jnp.zeros((MARGIN, cols), jnp.float32)

        def fill(owner, carry):
            start = pl.multiple_of(owner * rows + MARGIN, MARGIN)
            first = pl.multiple_of(owner * rows, rows)
            for band in range(bands):
                framed[band, pl.ds(start, rows), :] = template[owner, band].astype(jnp.float32)
                sums[band, pl.ds(first, rows), :] = jnp.zeros((rows, cols), jnp.float32)
            return carry

        lax.fori_loop(0, owners, fill, 0)
        for band in range(bands):
            tail = jnp.zeros((2 * MARGIN, cols), jnp.float32)
            sums[band, ends - 2 * MARGIN : ends, :] = tail

    def one(slot, carry):
        at = step * slots + slot
        first = pl.multiple_of(ints[at], ROW_BLOCK)
        source = columns[slot].reshape(bands * rows, cols)
        warped = jnp.dot(tables[slot], source, preferred_element_type=jnp.float32)
        for block in range(canvas_rows // ROW_BLOCK):
            low = block * ROW_BLOCK
            cover_rows = row_cover[slot, low : low + ROW_BLOCK, :]
            cover_rows = jnp.concatenate([cover_rows] * (cols // LANES), axis=1)
            weight = cover_rows * plane[slot, block : block + 1, :]
            for band in range(bands):
                where = pl.ds(first + low, ROW_BLOCK)
                base = band * canvas_rows + low
                prior = framed[band, where, :]
                inverse = floats[(at * bands + band) * 3]
                over = floats[(at * bands + band) * 3 + 1]
                ratio = floats[(at * bands + band) * 3 + 2]
                pull = jnp.tanh((warped[base : base + ROW_BLOCK, :] - prior) * inverse)
                sums[band, where, :] += weight * (prior * over + pull * ratio)
        return carry

    lax.fori_loop(0, slots, one, 0)

    @pl.when(step == pl.num_programs(0) - 1)
    def _():
        def give(owner, carry):
            start = pl.multiple_of(owner * rows + MARGIN, MARGIN)
            for band in range(bands):
                value = sums[band, pl.ds(start, rows), :].astype(out.dtype)
                for quarter in range(quarters):
                    part = value[:, quarter * width : (quarter + 1) * width]
                    out[quarter, owner, band] = part
            return carry

        lax.fori_loop(0, owners, give, 0)


def clip_and_sum(starts, scales, columns, tables, row_cover, plane, template, quarters):
    held, bands, rows, cols = columns.shape
    owners = template.shape[0]
    canvas_rows = row_cover.shape[1]
    height = owners * rows + 2 * MARGIN
    out_shape = (quarters, owners, bands, rows, cols // quarters)

    def by_slot(*shape):
        return pl.BlockSpec((GROUP,) + shape, lambda g: (g,) + (0,) * len(shape))

    return pl.pallas_call(
        clip_kernel,
        grid=(held // GROUP,),
        out_shape=jax.ShapeDtypeStruct(out_shape, jnp.bfloat16),
        in_specs=[
            pl.BlockSpec(memory_space=pltpu.SMEM),
            pl.BlockSpec(memory_space=pltpu.SMEM),
            by_slot(bands, rows, cols),
            by_slot(*tables.shape[1:]),
            by_slot(*row_cover.shape[1:]),
            by_slot(*plane.shape[1:]),
            pl.BlockSpec(template.shape, lambda g: (0, 0, 0, 0)),
        ],
        out_specs=pl.BlockSpec(out_shape, lambda g: (0, 0, 0, 0, 0)),
        scratch_shapes=[
            pltpu.VMEM((bands, height, cols), jnp.float32),
            pltpu.VMEM((bands, height, cols), jnp.float32),
        ],
        compiler_params=pltpu.CompilerParams(
            dimension_semantics=("arbitrary",), vmem_limit_bytes=48 * 1024 * 1024
        ),
        cost_estimate=pl.CostEstimate(
            flops=20 * held * bands * canvas_rows * cols,
            bytes_accessed=2 * held * bands * rows * cols,
            transcendentals=held * bands * canvas_rows * cols,
        ),
        name="clip",
    )(starts, scales, columns, tables, row_cover, plane, template)


def row_tables(shifts, taps, bands, rows, canvas_rows):
    shape = (1, bands * canvas_rows, bands * rows)
    i = lax.broadcasted_iota(jnp.int32, shape, 1)
    k = lax.broadcasted_iota(jnp.int32, shape, 2)
    gap = i % canvas_rows - MARGIN - k % rows - shifts[:, None, None]
    value = jnp.zeros(gap.shape, jnp.float32)
    for tap in range(TAPS):
        value = jnp.where(gap == 3 - tap, taps[:, tap][:, None, None], value)
    return jnp.where(i // canvas_rows == k // rows, value, 0.0).astype(jnp.bfloat16)


def spread(index, block_count, block):
    which = jnp.arange(block_count, dtype=jnp.int32)[:, None] == (index // block)[None, :]
    return which.astype(jnp.float32)


def on_device(
    slot_pixels,
    slot_tile,
    slot_offset,
    slot_frac,
    slot_sigma,
    clip_mask,
    slot_count,
    template,
    prior_weight,
):
    sky_count = lax.axis_size("sky")
    epoch_count = lax.axis_size("epoch")
    held, bands, rows, cols = slot_pixels.shape
    canvas_rows = rows + 2 * MARGIN
    row_blocks, col_blocks = clip_mask.shape[1:]
    part_width = cols // epoch_count
    high = lax.Precision.HIGHEST

    whole_template = lax.all_gather(template, "sky", axis=0, tiled=False)

    target = slot_tile[:, 0]
    shift_y, shift_x = slot_offset[:, 0], slot_offset[:, 1]
    taps = tap_weights(slot_frac.astype(jnp.float32))
    taps_y, taps_x = taps[:, 0], taps[:, 1]
    sigmas = slot_sigma.astype(jnp.float32)
    over = 1.0 / (sigmas * sigmas)
    live = (jnp.arange(held, dtype=jnp.int32) < slot_count[0]).astype(jnp.float32)
    masks = clip_mask.astype(jnp.float32) * live[:, None, None]

    columns = warp_columns(slot_pixels, shift_x, taps_x)

    row_index = jnp.arange(canvas_rows, dtype=jnp.int32) - MARGIN
    col_index = jnp.arange(cols, dtype=jnp.int32)
    row_cover = cover(shift_y, taps_y, row_index, rows)
    col_cover = cover(shift_x, taps_x, col_index, cols)
    expand = spread(col_index, col_blocks, cols // col_blocks)
    plane = jnp.einsum("sik,kj->sij", masks, expand, precision=high) * col_cover[:, None, :]
    tables = row_tables(shift_y, taps_y, bands, rows, canvas_rows)
    wide_cover = jnp.broadcast_to(row_cover[:, :, None], (held, canvas_rows, LANES))
    scale = CLIP_WIDTH * sigmas
    scales = jnp.stack([1.0 / scale, over, scale * over], 2).reshape(-1)

    block_rows = row_cover.reshape(held, row_blocks, canvas_rows // row_blocks).sum(2)
    block_cols = col_cover.reshape(held, col_blocks, cols // col_blocks).sum(2)
    block = jnp.arange(row_blocks, dtype=jnp.int32)[None, :]
    above = (target[:, None] == 0) & (block == 0)
    below = (target[:, None] == sky_count - 1) & (block == row_blocks - 1)
    block_rows = jnp.where(above | below, 0.0, block_rows)
    tile_total = jnp.sum(masks * block_rows[:, :, None] * block_cols[:, None, :], (1, 2))
    band_part = jnp.sum(tile_total[:, None] * over, 0)
    band_part = band_part + jnp.sum(prior_weight, 1) * (cols / epoch_count)

    owners = jnp.arange(sky_count, dtype=jnp.int32)
    onehot = (target[:, None] == owners[None, :]).astype(jnp.int32)
    rank = jnp.sum(jnp.cumsum(onehot, 0) * onehot, 1) - 1
    position = target * CAPACITY + rank
    routes = jnp.arange(sky_count * CAPACITY, dtype=jnp.int32)
    chooser = (position[None, :] == routes[:, None]).astype(jnp.float32)
    cells = row_blocks * col_blocks
    described = jnp.concatenate(
        [
            masks.reshape(held, cells),
            slot_offset.astype(jnp.float32),
            slot_frac.astype(jnp.float32),
            sigmas,
        ],
        1,
    )
    chosen = jnp.dot(chooser, described, precision=high)
    totals = jnp.broadcast_to(band_part[None, :], (chosen.shape[0], bands))
    message = jnp.concatenate([chosen, totals], 1)
    message = jnp.pad(message, ((0, 0), (0, LANES - message.shape[1])))
    message = message.reshape(sky_count, CAPACITY, LANES)
    arrived = lax.all_to_all(message, "sky", split_axis=0, concat_axis=0, tiled=True)
    arrived = lax.all_gather(arrived, "epoch", axis=0, tiled=True)
    band_total = jnp.sum(arrived[:, 0, cells + 4 + bands : cells + 4 + 2 * bands], 0)
    arrived = arrived.reshape(-1, LANES)

    epoch_position = lax.axis_index("epoch")
    own_masks = arrived[:, :cells].reshape(-1, row_blocks, col_blocks)
    own_shift = arrived[:, cells : cells + 2].astype(jnp.int32)
    own_taps = tap_weights(arrived[:, cells + 2 : cells + 4])
    own_sigmas = arrived[:, cells + 4 : cells + 4 + bands]
    own_sigmas = jnp.where(own_sigmas > 0.0, own_sigmas, 1.0)
    own_over = 1.0 / (own_sigmas * own_sigmas)
    own_index = epoch_position * part_width + jnp.arange(part_width, dtype=jnp.int32)
    own_rows = cover(own_shift[:, 0], own_taps[:, 0], row_index, rows)
    own_cols = cover(own_shift[:, 1], own_taps[:, 1], own_index, cols)
    own_expand = spread(own_index, col_blocks, cols // col_blocks)
    own_plane = jnp.einsum("sik,kj->isj", own_masks, own_expand, precision=high)
    own_plane = own_plane * own_cols[None]
    left = own_over[:, :, None, None] * own_rows.reshape(-1, 1, row_blocks, ROW_BLOCK)
    weights = jnp.einsum("sbir,isj->birj", left, own_plane, precision=high)
    weights = weights.reshape(bands, canvas_rows, part_width)
    ring = [(i, i + 1) for i in range(sky_count - 1)]
    from_above = lax.ppermute(weights[:, canvas_rows - MARGIN :], "sky", ring)
    from_below = lax.ppermute(weights[:, :MARGIN], "sky", [(j, i) for i, j in ring])
    weight_sum = weights[:, MARGIN : MARGIN + rows]
    weight_sum = weight_sum.at[:, :MARGIN].add(from_above)
    weight_sum = weight_sum.at[:, rows - MARGIN :].add(from_below)

    partial = clip_and_sum(
        target * rows, scales, columns, tables, wide_cover, plane, whole_template, epoch_count
    )
    flux = lax.psum_scatter(partial, "epoch", scatter_dimension=0, tiled=False)
    flux = lax.psum_scatter(flux, "sky", scatter_dimension=0, tiled=False)
    flux_sum = flux.astype(jnp.float32)

    template_part = lax.dynamic_slice_in_dim(
        template, epoch_position * part_width, part_width, 2
    ).astype(jnp.float32)
    prior = prior_weight[:, :, None]
    depth_map = weight_sum + prior
    coadd_image = ((flux_sum + prior * template_part) / depth_map).astype(jnp.bfloat16)
    band_mean = band_total / (rows * sky_count * cols)
    depth_norm = (depth_map / band_mean[:, None, None]).astype(jnp.bfloat16)
    return (coadd_image, depth_norm)


def solution(mesh):
    in_specs = (
        P(("groups", "sky", "epoch"), "band", None, None),
        P(("groups", "sky", "epoch"), None),
        P(("groups", "sky", "epoch"), None),
        P(("groups", "sky", "epoch"), None),
        P(("groups", "sky", "epoch"), "band"),
        P(("groups", "sky", "epoch"), None, None),
        P(("groups", "sky", "epoch")),
        P("band", ("groups", "sky"), None),
        P("band", ("groups", "sky")),
    )
    out_specs = (P("band", ("groups", "sky"), "epoch"), P("band", ("groups", "sky"), "epoch"))
    return jax.shard_map(
        on_device, mesh=mesh, in_specs=in_specs, out_specs=out_specs, check_vma=False
    )
```

```python
import functools

import jax
import jax.numpy as jnp
from jax import lax
from jax.experimental import pallas as pl
from jax.experimental.pallas import tpu as pltpu
from jax.sharding import PartitionSpec as P


MARGIN = 8
CAPACITY = 2
CLIP_WIDTH = 3.0
TAPS = 6
ROW_BLOCK = 8
LANES = 128
GROUP = 8
CLIP_GROUP = 48
UNROLL = 4
NEAR = 4


def lanczos(distance):
    inside = jnp.abs(distance) < 3.0
    return jnp.where(inside, jnp.sinc(distance) * jnp.sinc(distance / 3.0), 0.0)


def tap_weights(fractions):
    gaps = 3.0 - jnp.arange(TAPS, dtype=jnp.float32)
    rounded = lanczos(gaps - fractions[..., None]).astype(jnp.bfloat16)
    return lax.optimization_barrier(rounded).astype(jnp.float32)


def cover(shifts, taps, index, length_in):
    total = jnp.zeros((shifts.shape[0], index.shape[0]), jnp.float32)
    for tap in range(TAPS):
        source = index[None, :] - shifts[:, None] + (tap - 3)
        inside = (source >= 0) & (source < length_in)
        total = total + jnp.where(inside, taps[:, tap][:, None], 0.0)
    return jnp.clip(total, 0.0, 1.0)


def column_kernel(ints, floats, after, pixels, out, tables):
    step = pl.program_id(0)
    slots, bands, rows, cols = pixels.shape
    blocks = cols // LANES
    edge = 16
    parts = out.shape[0]
    width = cols // parts

    @pl.when(step == 0)
    def _():
        tables[...] = jnp.zeros_like(tables)

    def gap_base(first_row, count, offset):
        k = lax.broadcasted_iota(jnp.int32, (count, LANES), 0) + first_row
        j = lax.broadcasted_iota(jnp.int32, (count, LANES), 1)
        return j - k + offset

    def one(slot, table):
        at = step * slots + slot
        shift = ints[at]
        weights = [floats[at * TAPS + tap] for tap in range(TAPS)]

        def band_of(base):
            gap = base - shift
            value = jnp.zeros(base.shape, jnp.float32)
            for tap in range(TAPS):
                value = jnp.where(gap == 3 - tap, weights[tap], value)
            return value.astype(jnp.bfloat16)

        diagonal = band_of(gap_base(0, LANES, 0))
        upper = band_of(gap_base(LANES - edge, edge, LANES))
        lower = band_of(gap_base(0, edge, -LANES))
        for block in range(blocks):
            low, high = block * LANES, (block + 1) * LANES
            table[low:high, low:high] = diagonal
            if block + 1 < blocks:
                table[high - edge : high, high : high + LANES] = upper
                table[high : high + edge, low:high] = lower
        source = pixels[slot].reshape(bands * rows, cols)
        warped = jnp.dot(source, table[...], preferred_element_type=jnp.float32)
        warped = warped.astype(out.dtype)
        for part in range(parts):
            for band in range(bands):
                piece = warped[band * rows : (band + 1) * rows, part * width : (part + 1) * width]
                out[part, slot, :, band * width : (band + 1) * width] = piece

    def pair(index, carry):
        for half in range(2):
            one(index * 2 + half, tables.at[half])
        return carry

    lax.fori_loop(0, slots // 2, pair, 0)


def warp_columns(pixels, shifts, taps, after, parts):
    held, bands, rows, cols = pixels.shape
    width = bands * cols // parts
    return pl.pallas_call(
        column_kernel,
        grid=(held // GROUP,),
        out_shape=jax.ShapeDtypeStruct((parts, held, rows, width), jnp.bfloat16),
        in_specs=[
            pl.BlockSpec(memory_space=pltpu.SMEM),
            pl.BlockSpec(memory_space=pltpu.SMEM),
            pl.BlockSpec(memory_space=pl.ANY),
            pl.BlockSpec((GROUP, bands, rows, cols), lambda g: (g, 0, 0, 0)),
        ],
        out_specs=pl.BlockSpec((parts, GROUP, rows, width), lambda g: (0, g, 0, 0)),
        scratch_shapes=[pltpu.VMEM((2, cols, cols), jnp.bfloat16)],
        compiler_params=pltpu.CompilerParams(dimension_semantics=("arbitrary",)),
        cost_estimate=pl.CostEstimate(
            flops=2 * held * bands * rows * cols * cols,
            bytes_accessed=4 * held * bands * rows * cols,
            transcendentals=0,
        ),
        name="columns",
    )(shifts, taps.reshape(-1), after, pixels)


def clip_kernel(ints, floats, columns, plane, template, out, framed, sums):
    step = pl.program_id(0)
    slots, rows, width = columns.shape
    owners = out.shape[0]
    bands = width // LANES
    canvas_rows = rows + 2 * MARGIN
    total = pl.num_programs(0) * slots

    @pl.when(step == 0)
    def _():
        ends = framed.shape[0]
        framed[0:MARGIN, :] = jnp.zeros((MARGIN, width), jnp.float32)
        framed[ends - MARGIN : ends, :] = jnp.zeros((MARGIN, width), jnp.float32)

        def fill(owner, carry):
            start = pl.multiple_of(owner * rows + MARGIN, MARGIN)
            first = pl.multiple_of(owner * rows, rows)
            framed[pl.ds(start, rows), :] = template[owner, 0:rows, :].astype(jnp.float32)
            sums[pl.ds(first, rows), :] = jnp.zeros((rows, width), jnp.float32)
            return carry

        lax.fori_loop(0, owners, fill, 0)
        sums[ends - 2 * MARGIN : ends, :] = jnp.zeros((2 * MARGIN, width), jnp.float32)

    i = lax.broadcasted_iota(jnp.int32, (canvas_rows, LANES), 0)
    k = lax.broadcasted_iota(jnp.int32, (canvas_rows, LANES), 1)
    base = i - MARGIN - k
    ones = jnp.ones((rows, LANES), columns.dtype)

    def one(slot):
        at = step * slots + slot
        first = pl.multiple_of(ints[at], ROW_BLOCK)
        gap = base - ints[total + at]
        table = jnp.zeros(gap.shape, jnp.float32)
        per_slot = TAPS + 3 * bands
        for tap in range(TAPS):
            table = jnp.where(gap == 3 - tap, floats[at * per_slot + tap], table)
        table = table.astype(columns.dtype)[:, :rows]
        source = jnp.concatenate([columns[slot], ones], axis=1)
        warped = jnp.dot(table, source, preferred_element_type=jnp.float32)
        for block in range(canvas_rows // ROW_BLOCK):
            low = block * ROW_BLOCK
            where = pl.ds(first + low, ROW_BLOCK)
            row_cover = jnp.clip(warped[low : low + ROW_BLOCK, width:], 0.0, 1.0)
            weight = row_cover * plane[slot, block : block + 1, :]
            for band in range(bands):
                lanes = slice(band * LANES, (band + 1) * LANES)
                prior = framed[where, lanes]
                scale = at * per_slot + TAPS + 3 * band
                pull = (warped[low : low + ROW_BLOCK, lanes] - prior) * floats[scale]
                value = prior * floats[scale + 1] + jnp.tanh(pull) * floats[scale + 2]
                sums[where, lanes] += weight * value

    def several(index, carry):
        for part in range(UNROLL):
            one(index * UNROLL + part)
        return carry

    lax.fori_loop(0, slots // UNROLL, several, 0)

    @pl.when(step == pl.num_programs(0) - 1)
    def _():
        def give(owner, carry):
            start = pl.multiple_of(owner * rows + MARGIN, MARGIN)
            out[owner] = sums[pl.ds(start, rows), :].astype(out.dtype)
            return carry

        lax.fori_loop(0, owners, give, 0)


def clip_and_sum(ints, floats, columns, plane, template):
    tiles, rows, width = columns.shape
    owners = template.shape[0]
    height = owners * rows + 2 * MARGIN
    out_shape = (owners, rows, width)
    return pl.pallas_call(
        clip_kernel,
        grid=(tiles // CLIP_GROUP,),
        out_shape=jax.ShapeDtypeStruct(out_shape, jnp.bfloat16),
        in_specs=[
            pl.BlockSpec(memory_space=pltpu.SMEM),
            pl.BlockSpec(memory_space=pltpu.SMEM),
            pl.BlockSpec((CLIP_GROUP, rows, width), lambda g: (g, 0, 0)),
            pl.BlockSpec((CLIP_GROUP,) + plane.shape[1:], lambda g: (g, 0, 0)),
            pl.BlockSpec(template.shape, lambda g: (0, 0, 0)),
        ],
        out_specs=pl.BlockSpec(out_shape, lambda g: (0, 0, 0)),
        scratch_shapes=[
            pltpu.VMEM((height, width), jnp.float32),
            pltpu.VMEM((height, width), jnp.float32),
        ],
        compiler_params=pltpu.CompilerParams(
            dimension_semantics=("arbitrary",), vmem_limit_bytes=32 * 1024 * 1024
        ),
        cost_estimate=pl.CostEstimate(
            flops=30 * tiles * (rows + 2 * MARGIN) * width,
            bytes_accessed=2 * tiles * rows * width,
            transcendentals=tiles * (rows + 2 * MARGIN) * width,
        ),
        name="clip",
    )(ints, floats, columns, plane, template)


def spread(index, block_count, block):
    which = jnp.arange(block_count, dtype=jnp.int32)[:, None] == (index // block)[None, :]
    return which.astype(jnp.float32)


def summed_on_arrival(parts, axis, groups=None):
    arrived = lax.all_to_all(
        parts, axis, split_axis=0, concat_axis=0, tiled=True, axis_index_groups=groups
    )
    return functools.reduce(jnp.add, [part.astype(jnp.float32) for part in arrived])


def sum_over_sky(parts):
    count = parts.shape[0]
    if NEAR == 1 or count % NEAR:
        return summed_on_arrival(parts, "sky")
    far = count // NEAR
    near_groups = [[f * NEAR + n for n in range(NEAR)] for f in range(far)]
    far_groups = [[f * NEAR + n for f in range(far)] for n in range(NEAR)]
    parts = jnp.swapaxes(parts.reshape((far, NEAR) + parts.shape[1:]), 0, 1)
    parts = summed_on_arrival(parts, "sky", near_groups).astype(jnp.bfloat16)
    return summed_on_arrival(parts, "sky", far_groups)


def on_device(
    slot_pixels,
    slot_tile,
    slot_offset,
    slot_frac,
    slot_sigma,
    clip_mask,
    slot_count,
    template,
    prior_weight,
):
    sky_count = lax.axis_size("sky")
    epoch_count = lax.axis_size("epoch")
    epoch_position = lax.axis_index("epoch")
    held, bands, rows, cols = slot_pixels.shape
    canvas_rows = rows + 2 * MARGIN
    row_blocks, col_blocks = clip_mask.shape[1:]
    cells = row_blocks * col_blocks
    part_width = cols // epoch_count
    high = lax.Precision.HIGHEST

    template_part = lax.dynamic_slice_in_dim(
        template, epoch_position * part_width, part_width, 2
    )
    sent = jnp.swapaxes(template_part, 0, 1).reshape(rows, bands * part_width)
    sent = jnp.pad(sent, ((0, rows // 2), (0, 0)))
    whole_template = lax.all_gather(sent, "sky", axis=0, tiled=False)

    taps_x = tap_weights(slot_frac[:, 1].astype(jnp.float32))
    columns = warp_columns(slot_pixels, slot_offset[:, 1], taps_x, sent, epoch_count)
    columns = lax.all_to_all(columns, "epoch", split_axis=0, concat_axis=0, tiled=True)
    columns = columns.reshape((-1,) + columns.shape[2:])

    live = (jnp.arange(held, dtype=jnp.int32) < slot_count[0]).astype(jnp.float32)
    described = jnp.concatenate(
        [
            clip_mask.astype(jnp.float32).reshape(held, cells) * live[:, None],
            slot_offset.astype(jnp.float32),
            slot_frac.astype(jnp.float32),
            slot_sigma.astype(jnp.float32),
            slot_tile.astype(jnp.float32),
        ],
        1,
    )
    described = jnp.pad(described, ((0, 0), (0, LANES - described.shape[1])))
    described = lax.all_gather(described, "epoch", axis=0, tiled=True)
    tiles = described.shape[0]

    def unpack(table):
        masks = table[:, :cells].reshape(-1, row_blocks, col_blocks)
        shifts = table[:, cells : cells + 2].astype(jnp.int32)
        taps = tap_weights(table[:, cells + 2 : cells + 4])
        sigmas = table[:, cells + 4 : cells + 4 + bands]
        sigmas = jnp.where(sigmas > 0.0, sigmas, 1.0)
        return masks, shifts, taps, sigmas

    row_index = jnp.arange(canvas_rows, dtype=jnp.int32) - MARGIN
    col_index = epoch_position * part_width + jnp.arange(part_width, dtype=jnp.int32)
    all_index = jnp.arange(cols, dtype=jnp.int32)
    expand = spread(col_index, col_blocks, cols // col_blocks)

    masks, shifts, taps, sigmas = unpack(described)
    target = described[:, cells + 4 + bands].astype(jnp.int32)
    over = 1.0 / (sigmas * sigmas)
    row_cover = cover(shifts[:, 0], taps[:, 0], row_index, rows)
    col_cover = cover(shifts[:, 1], taps[:, 1], all_index, cols)
    own_cover = lax.dynamic_slice_in_dim(col_cover, epoch_position * part_width, part_width, 1)
    plane = jnp.einsum("sik,kj->sij", masks, expand, precision=high) * own_cover[:, None, :]
    scale = CLIP_WIDTH * sigmas
    scales = jnp.stack([1.0 / scale, over, scale * over], 2).reshape(tiles, 3 * bands)
    floats = jnp.concatenate([taps[:, 0], scales], 1).reshape(-1)
    ints = jnp.concatenate([target * rows, shifts[:, 0]])

    block_rows = row_cover.reshape(tiles, row_blocks, canvas_rows // row_blocks).sum(2)
    block_cols = col_cover.reshape(tiles, col_blocks, cols // col_blocks).sum(2)
    block = jnp.arange(row_blocks, dtype=jnp.int32)[None, :]
    above = (target[:, None] == 0) & (block == 0)
    below = (target[:, None] == sky_count - 1) & (block == row_blocks - 1)
    block_rows = jnp.where(above | below, 0.0, block_rows)
    tile_total = jnp.sum(masks * block_rows[:, :, None] * block_cols[:, None, :], (1, 2))
    band_part = jnp.sum(tile_total[:, None] * over, 0) + jnp.sum(prior_weight, 1) * cols

    owners = jnp.arange(sky_count, dtype=jnp.int32)
    onehot = (target[:, None] == owners[None, :]).astype(jnp.int32)
    onehot = onehot.reshape(epoch_count, held, sky_count)
    rank = jnp.sum(jnp.cumsum(onehot, 1) * onehot, 2) - 1
    rank = rank + CAPACITY * jnp.arange(epoch_count, dtype=jnp.int32)[:, None]
    routes = CAPACITY * epoch_count
    position = target * routes + rank.reshape(-1)
    slots = jnp.arange(sky_count * routes, dtype=jnp.int32)
    chooser = (position[None, :] == slots[:, None]).astype(jnp.float32)
    chosen = jnp.dot(chooser, described[:, : cells + 4 + bands], precision=high)
    totals = jnp.broadcast_to(band_part[None, :], (chosen.shape[0], bands))
    message = jnp.concatenate([chosen, totals], 1)
    message = jnp.pad(message, ((0, 0), (0, LANES - message.shape[1])))
    message = message.reshape(sky_count, routes, LANES)
    arrived = lax.all_to_all(message, "sky", split_axis=0, concat_axis=0, tiled=True)
    band_total = jnp.sum(arrived[:, 0, cells + 4 + bands : cells + 4 + 2 * bands], 0)

    own_masks, own_shift, own_taps, own_sigmas = unpack(arrived.reshape(-1, LANES))
    own_over = 1.0 / (own_sigmas * own_sigmas)
    own_rows = cover(own_shift[:, 0], own_taps[:, 0], row_index, rows)
    own_cols = cover(own_shift[:, 1], own_taps[:, 1], col_index, cols)
    own_plane = jnp.einsum("sik,kj->isj", own_masks, expand, precision=high) * own_cols[None]
    left = own_over[:, :, None, None] * own_rows.reshape(-1, 1, row_blocks, ROW_BLOCK)
    weights = jnp.einsum("sbir,isj->birj", left, own_plane, precision=high)
    weights = weights.reshape(bands, canvas_rows, part_width)
    ring = [(i, i + 1) for i in range(sky_count - 1)]
    from_above = lax.ppermute(weights[:, canvas_rows - MARGIN :], "sky", ring)
    from_below = lax.ppermute(weights[:, :MARGIN], "sky", [(j, i) for i, j in ring])
    weight_sum = weights[:, MARGIN : MARGIN + rows]
    weight_sum = weight_sum.at[:, :MARGIN].add(from_above)
    weight_sum = weight_sum.at[:, rows - MARGIN :].add(from_below)

    flux = sum_over_sky(clip_and_sum(ints, floats, columns, plane, whole_template))
    flux_sum = jnp.swapaxes(flux.reshape(rows, bands, part_width), 0, 1)

    prior = prior_weight[:, :, None]
    depth_map = weight_sum + prior
    coadd_image = (flux_sum + prior * template_part.astype(jnp.float32)) / depth_map
    band_mean = band_total / (rows * sky_count * cols)
    depth_norm = (depth_map / band_mean[:, None, None]).astype(jnp.bfloat16)
    return (coadd_image.astype(jnp.bfloat16), depth_norm)


def solution(mesh):
    in_specs = (
        P(("groups", "sky", "epoch"), "band", None, None),
        P(("groups", "sky", "epoch"), None),
        P(("groups", "sky", "epoch"), None),
        P(("groups", "sky", "epoch"), None),
        P(("groups", "sky", "epoch"), "band"),
        P(("groups", "sky", "epoch"), None, None),
        P(("groups", "sky", "epoch")),
        P("band", ("groups", "sky"), None),
        P("band", ("groups", "sky")),
    )
    out_specs = (P("band", ("groups", "sky"), "epoch"), P("band", ("groups", "sky"), "epoch"))
    return jax.shard_map(
        on_device, mesh=mesh, in_specs=in_specs, out_specs=out_specs, check_vma=False
    )
```

```python
import functools

import jax
import jax.numpy as jnp
from jax import lax
from jax.experimental import pallas as pl
from jax.experimental.pallas import tpu as pltpu
from jax.sharding import PartitionSpec as P


MARGIN = 8
CAPACITY = 2
CLIP_WIDTH = 3.0
TAPS = 6
ROW_BLOCK = 8
LANES = 128
GROUP = 8
UNROLL = 4
NEAR = 4


def lanczos(distance):
    inside = jnp.abs(distance) < 3.0
    return jnp.where(inside, jnp.sinc(distance) * jnp.sinc(distance / 3.0), 0.0)


def tap_weights(fractions):
    gaps = 3.0 - jnp.arange(TAPS, dtype=jnp.float32)
    rounded = lanczos(gaps - fractions[..., None]).astype(jnp.bfloat16)
    return lax.optimization_barrier(rounded).astype(jnp.float32)


def cover(shifts, taps, index, length_in):
    total = jnp.zeros((shifts.shape[0], index.shape[0]), jnp.float32)
    for tap in range(TAPS):
        source = index[None, :] - shifts[:, None] + (tap - 3)
        inside = (source >= 0) & (source < length_in)
        total = total + jnp.where(inside, taps[:, tap][:, None], 0.0)
    return jnp.clip(total, 0.0, 1.0)


def column_kernel(ints, floats, pixels, out, tables):
    step = pl.program_id(0)
    slots, bands, rows, cols = pixels.shape
    blocks = cols // LANES
    edge = 16
    turn = ints[pl.num_programs(0) * slots]
    parts = out.shape[0]
    width = cols // parts

    @pl.when(step == 0)
    def _():
        tables[...] = jnp.zeros_like(tables)

    def gap_base(first_row, count, offset):
        k = lax.broadcasted_iota(jnp.int32, (count, LANES), 0) + first_row
        j = lax.broadcasted_iota(jnp.int32, (count, LANES), 1)
        return j - k + offset

    def one(slot, table):
        at = step * slots + slot
        shift = ints[at]
        weights = [floats[at * TAPS + tap] for tap in range(TAPS)]

        def band_of(base):
            gap = base - shift
            value = jnp.zeros(base.shape, jnp.float32)
            for tap in range(TAPS):
                value = jnp.where(gap == 3 - tap, weights[tap], value)
            return value.astype(jnp.bfloat16)

        diagonal = band_of(gap_base(0, LANES, 0))
        upper = band_of(gap_base(LANES - edge, edge, LANES))
        lower = band_of(gap_base(0, edge, -LANES))
        for block in range(blocks):
            low, high = block * LANES, (block + 1) * LANES
            table[low:high, low:high] = diagonal
            if block + 1 < blocks:
                table[high - edge : high, high : high + LANES] = upper
                table[high : high + edge, low:high] = lower
        source = pixels[slot].reshape(bands * rows, cols)
        warped = jnp.dot(source, table[...], preferred_element_type=jnp.float32)
        warped = warped.astype(out.dtype)
        for part in range(parts):
            ahead = lax.rem(part - turn + parts, parts)
            for band in range(bands):
                piece = warped[band * rows : (band + 1) * rows, part * width : (part + 1) * width]
                out[ahead, slot, :, band * width : (band + 1) * width] = piece

    def pair(index, carry):
        for half in range(2):
            one(index * 2 + half, tables.at[half])
        return carry

    lax.fori_loop(0, slots // 2, pair, 0)


def warp_columns(pixels, shifts, taps, turn, parts):
    held, bands, rows, cols = pixels.shape
    width = bands * cols // parts
    return pl.pallas_call(
        column_kernel,
        grid=(held // GROUP,),
        out_shape=jax.ShapeDtypeStruct((parts, held, rows, width), jnp.bfloat16),
        in_specs=[
            pl.BlockSpec(memory_space=pltpu.SMEM),
            pl.BlockSpec(memory_space=pltpu.SMEM),
            pl.BlockSpec((GROUP, bands, rows, cols), lambda g: (g, 0, 0, 0)),
        ],
        out_specs=pl.BlockSpec((parts, GROUP, rows, width), lambda g: (0, g, 0, 0)),
        scratch_shapes=[pltpu.VMEM((2, cols, cols), jnp.bfloat16)],
        compiler_params=pltpu.CompilerParams(dimension_semantics=("arbitrary",)),
        cost_estimate=pl.CostEstimate(
            flops=2 * held * bands * rows * cols * cols,
            bytes_accessed=4 * held * bands * rows * cols,
            transcendentals=0,
        ),
        name="columns",
    )(jnp.append(shifts, turn), taps.reshape(-1), pixels)


def clip_kernel(ints, floats, plane, template, *refs):
    groups, (out, framed, sums) = refs[:-3], refs[-3:]
    slots, rows, width = groups[0].shape
    owners = out.shape[0]
    near = template.shape[0]
    bands = width // LANES
    canvas_rows = rows + 2 * MARGIN
    total = len(groups) * slots
    ends = framed.shape[0]
    framed[0:MARGIN, :] = jnp.zeros((MARGIN, width), jnp.float32)
    framed[ends - MARGIN : ends, :] = jnp.zeros((MARGIN, width), jnp.float32)

    def fill(owner, carry):
        start = pl.multiple_of(owner * rows + MARGIN, MARGIN)
        first = pl.multiple_of(owner * rows, rows)
        block = template[lax.rem(owner, near), lax.div(owner, near)]
        framed[pl.ds(start, rows), :] = block.astype(jnp.float32)
        sums[pl.ds(first, rows), :] = jnp.zeros((rows, width), jnp.float32)
        return carry

    lax.fori_loop(0, owners, fill, 0)
    sums[ends - 2 * MARGIN : ends, :] = jnp.zeros((2 * MARGIN, width), jnp.float32)

    i = lax.broadcasted_iota(jnp.int32, (canvas_rows, LANES), 0)
    k = lax.broadcasted_iota(jnp.int32, (canvas_rows, LANES), 1)
    base = i - MARGIN - k
    ones = jnp.ones((rows, LANES), out.dtype)

    def one(group, slot):
        columns = groups[group]
        at = group * slots + slot
        first = pl.multiple_of(ints[at], ROW_BLOCK)
        gap = base - ints[total + at]
        table = jnp.zeros(gap.shape, jnp.float32)
        per_slot = TAPS + 3 * bands
        for tap in range(TAPS):
            table = jnp.where(gap == 3 - tap, floats[at * per_slot + tap], table)
        table = table.astype(columns.dtype)[:, :rows]
        source = jnp.concatenate([columns[slot], ones], axis=1)
        warped = jnp.dot(table, source, preferred_element_type=jnp.float32)
        for block in range(canvas_rows // ROW_BLOCK):
            low = block * ROW_BLOCK
            where = pl.ds(first + low, ROW_BLOCK)
            row_cover = jnp.clip(warped[low : low + ROW_BLOCK, width:], 0.0, 1.0)
            weight = row_cover * plane[at, block : block + 1, :]
            for band in range(bands):
                lanes = slice(band * LANES, (band + 1) * LANES)
                prior = framed[where, lanes]
                scale = at * per_slot + TAPS + 3 * band
                pull = (warped[low : low + ROW_BLOCK, lanes] - prior) * floats[scale]
                value = prior * floats[scale + 1] + jnp.tanh(pull) * floats[scale + 2]
                sums[where, lanes] += weight * value

    def several(group, index, carry):
        for part in range(UNROLL):
            one(group, index * UNROLL + part)
        return carry

    for group in range(len(groups)):
        lax.fori_loop(0, slots // UNROLL, functools.partial(several, group), 0)

    def give(owner, carry):
        start = pl.multiple_of(owner * rows + MARGIN, MARGIN)
        out[owner] = sums[pl.ds(start, rows), :].astype(out.dtype)
        return carry

    lax.fori_loop(0, owners, give, 0)


def clip_and_sum(ints, floats, columns, plane, template):
    rows, width = columns[0].shape[1:]
    tiles = plane.shape[0]
    owners = template.shape[0] * template.shape[1]
    height = owners * rows + 2 * MARGIN
    out_shape = (owners, rows, width)
    return pl.pallas_call(
        clip_kernel,
        out_shape=jax.ShapeDtypeStruct(out_shape, jnp.bfloat16),
        in_specs=[pl.BlockSpec(memory_space=pltpu.SMEM)] * 2
        + [pl.BlockSpec(memory_space=pltpu.VMEM)] * (2 + len(columns)),
        out_specs=pl.BlockSpec(memory_space=pltpu.VMEM),
        scratch_shapes=[
            pltpu.VMEM((height, width), jnp.float32),
            pltpu.VMEM((height, width), jnp.float32),
        ],
        compiler_params=pltpu.CompilerParams(vmem_limit_bytes=32 * 1024 * 1024),
        cost_estimate=pl.CostEstimate(
            flops=30 * tiles * (rows + 2 * MARGIN) * width,
            bytes_accessed=2 * tiles * rows * width,
            transcendentals=tiles * (rows + 2 * MARGIN) * width,
        ),
        name="clip",
    )(ints, floats, plane, template, *columns)


def spread(index, block_count, block):
    which = jnp.arange(block_count, dtype=jnp.int32)[:, None] == (index // block)[None, :]
    return which.astype(jnp.float32)


def summed_on_arrival(parts, axis, groups=None):
    arrived = lax.all_to_all(
        parts, axis, split_axis=0, concat_axis=0, tiled=True, axis_index_groups=groups
    )
    return functools.reduce(jnp.add, [part.astype(jnp.float32) for part in arrived])


def sky_groups():
    count = lax.axis_size("sky")
    near = NEAR if count % NEAR == 0 else 1
    far = count // near
    near_groups = [[f * near + n for n in range(near)] for f in range(far)]
    far_groups = [[f * near + n for f in range(far)] for n in range(near)]
    return near, far, near_groups, far_groups


def sum_over_sky(parts):
    near, far, near_groups, far_groups = sky_groups()
    parts = jnp.swapaxes(parts.reshape((far, near) + parts.shape[1:]), 0, 1)
    parts = summed_on_arrival(parts, "sky", near_groups).astype(jnp.bfloat16)
    return summed_on_arrival(parts, "sky", far_groups)


def gather_over_sky(shard):
    near, far, near_groups, far_groups = sky_groups()

    def to_all(array, count, groups):
        copies = jnp.broadcast_to(array[None], (count,) + array.shape)
        return lax.all_to_all(
            copies, "sky", split_axis=0, concat_axis=0, tiled=True, axis_index_groups=groups
        )

    shard = to_all(shard, far, far_groups)
    return to_all(shard, near, near_groups)


def from_epochs(pieces):
    count = lax.axis_size("epoch")
    arrived = [pieces[0]]
    for ahead in range(1, count):
        route = [(i, (i + ahead) % count) for i in range(count)]
        arrived.append(lax.ppermute(pieces[ahead], "epoch", route))
    return arrived


def on_device(
    slot_pixels,
    slot_tile,
    slot_offset,
    slot_frac,
    slot_sigma,
    clip_mask,
    slot_count,
    template,
    prior_weight,
):
    sky_count = lax.axis_size("sky")
    epoch_count = lax.axis_size("epoch")
    epoch_position = lax.axis_index("epoch")
    held, bands, rows, cols = slot_pixels.shape
    canvas_rows = rows + 2 * MARGIN
    row_blocks, col_blocks = clip_mask.shape[1:]
    cells = row_blocks * col_blocks
    part_width = cols // epoch_count
    high = lax.Precision.HIGHEST

    template_part = lax.dynamic_slice_in_dim(
        template, epoch_position * part_width, part_width, 2
    )
    sent = jnp.swapaxes(template_part, 0, 1).reshape(rows, bands * part_width)
    whole_template = gather_over_sky(sent)

    live = (jnp.arange(held, dtype=jnp.int32) < slot_count[0]).astype(jnp.float32)
    described = jnp.concatenate(
        [
            clip_mask.astype(jnp.float32).reshape(held, cells) * live[:, None],
            slot_offset.astype(jnp.float32),
            slot_frac.astype(jnp.float32),
            slot_sigma.astype(jnp.float32),
            slot_tile.astype(jnp.float32),
        ],
        1,
    )
    described = jnp.pad(described, ((0, 0), (0, LANES - described.shape[1])))
    described = jnp.concatenate(from_epochs([described] * epoch_count), 0)
    tiles = described.shape[0]

    taps_x = tap_weights(slot_frac[:, 1].astype(jnp.float32))
    columns = warp_columns(slot_pixels, slot_offset[:, 1], taps_x, epoch_position, epoch_count)
    columns = from_epochs(columns)

    def unpack(table):
        masks = table[:, :cells].reshape(-1, row_blocks, col_blocks)
        shifts = table[:, cells : cells + 2].astype(jnp.int32)
        taps = tap_weights(table[:, cells + 2 : cells + 4])
        sigmas = table[:, cells + 4 : cells + 4 + bands]
        sigmas = jnp.where(sigmas > 0.0, sigmas, 1.0)
        return masks, shifts, taps, sigmas

    row_index = jnp.arange(canvas_rows, dtype=jnp.int32) - MARGIN
    col_index = epoch_position * part_width + jnp.arange(part_width, dtype=jnp.int32)
    all_index = jnp.arange(cols, dtype=jnp.int32)
    expand = spread(col_index, col_blocks, cols // col_blocks)

    masks, shifts, taps, sigmas = unpack(described)
    target = described[:, cells + 4 + bands].astype(jnp.int32)
    over = 1.0 / (sigmas * sigmas)
    row_cover = cover(shifts[:, 0], taps[:, 0], row_index, rows)
    col_cover = cover(shifts[:, 1], taps[:, 1], all_index, cols)
    own_cover = lax.dynamic_slice_in_dim(col_cover, epoch_position * part_width, part_width, 1)
    plane = jnp.einsum("sik,kj->sij", masks, expand, precision=high) * own_cover[:, None, :]
    scale = CLIP_WIDTH * sigmas
    scales = jnp.stack([1.0 / scale, over, scale * over], 2).reshape(tiles, 3 * bands)
    floats = jnp.concatenate([taps[:, 0], scales], 1).reshape(-1)
    ints = jnp.concatenate([target * rows, shifts[:, 0]])

    block_rows = row_cover.reshape(tiles, row_blocks, canvas_rows // row_blocks).sum(2)
    block_cols = col_cover.reshape(tiles, col_blocks, cols // col_blocks).sum(2)
    block = jnp.arange(row_blocks, dtype=jnp.int32)[None, :]
    above = (target[:, None] == 0) & (block == 0)
    below = (target[:, None] == sky_count - 1) & (block == row_blocks - 1)
    block_rows = jnp.where(above | below, 0.0, block_rows)
    tile_total = jnp.sum(masks * block_rows[:, :, None] * block_cols[:, None, :], (1, 2))
    band_part = jnp.sum(tile_total[:, None] * over, 0) + jnp.sum(prior_weight, 1) * cols

    owners = jnp.arange(sky_count, dtype=jnp.int32)
    onehot = (target[:, None] == owners[None, :]).astype(jnp.int32)
    onehot = onehot.reshape(epoch_count, held, sky_count)
    rank = jnp.sum(jnp.cumsum(onehot, 1) * onehot, 2) - 1
    rank = rank + CAPACITY * jnp.arange(epoch_count, dtype=jnp.int32)[:, None]
    routes = CAPACITY * epoch_count
    position = target * routes + rank.reshape(-1)
    slots = jnp.arange(sky_count * routes, dtype=jnp.int32)
    chooser = (position[None, :] == slots[:, None]).astype(jnp.float32)
    chosen = jnp.dot(chooser, described[:, : cells + 4 + bands], precision=high)
    pieces = []
    for _ in range(3):
        pieces.append(lax.reduce_precision(band_part, 8, 7))
        band_part = band_part - pieces[-1]
    totals = jnp.broadcast_to(jnp.concatenate(pieces)[None, :], (chosen.shape[0], 3 * bands))
    message = jnp.concatenate([chosen, totals], 1)
    message = jnp.pad(message, ((0, 0), (0, LANES - message.shape[1]))).astype(jnp.bfloat16)
    message = message.reshape(sky_count, routes, LANES)
    arrived = lax.all_to_all(message, "sky", split_axis=0, concat_axis=0, tiled=True)
    arrived = arrived.astype(jnp.float32)
    totals = arrived[:, 0, cells + 4 + bands : cells + 4 + 4 * bands]
    band_total = jnp.sum(totals.reshape(-1, bands), 0)

    own_masks, own_shift, own_taps, own_sigmas = unpack(arrived.reshape(-1, LANES))
    own_over = 1.0 / (own_sigmas * own_sigmas)
    own_rows = cover(own_shift[:, 0], own_taps[:, 0], row_index, rows)
    own_cols = cover(own_shift[:, 1], own_taps[:, 1], col_index, cols)
    own_plane = jnp.einsum("sik,kj->isj", own_masks, expand, precision=high) * own_cols[None]
    left = own_over[:, :, None, None] * own_rows.reshape(-1, 1, row_blocks, ROW_BLOCK)
    weights = jnp.einsum("sbir,isj->birj", left, own_plane, precision=high)
    weights = weights.reshape(bands, canvas_rows, part_width)
    ring = [(i, i + 1) for i in range(sky_count - 1)]
    from_above = lax.ppermute(weights[:, canvas_rows - MARGIN :], "sky", ring)
    from_below = lax.ppermute(weights[:, :MARGIN], "sky", [(j, i) for i, j in ring])
    weight_sum = weights[:, MARGIN : MARGIN + rows]
    weight_sum = weight_sum.at[:, :MARGIN].add(from_above)
    weight_sum = weight_sum.at[:, rows - MARGIN :].add(from_below)

    partial = clip_and_sum(ints, floats, columns, plane, whole_template)
    flux = sum_over_sky(partial)
    flux_sum = jnp.swapaxes(flux.reshape(rows, bands, part_width), 0, 1)

    prior = prior_weight[:, :, None]
    depth_map = weight_sum + prior
    coadd_image = (flux_sum + prior * template_part.astype(jnp.float32)) / depth_map
    band_mean = band_total / (rows * sky_count * cols)
    depth_norm = (depth_map / band_mean[:, None, None]).astype(jnp.bfloat16)
    return (coadd_image.astype(jnp.bfloat16), depth_norm)


def solution(mesh):
    in_specs = (
        P(("groups", "sky", "epoch"), "band", None, None),
        P(("groups", "sky", "epoch"), None),
        P(("groups", "sky", "epoch"), None),
        P(("groups", "sky", "epoch"), None),
        P(("groups", "sky", "epoch"), "band"),
        P(("groups", "sky", "epoch"), None, None),
        P(("groups", "sky", "epoch")),
        P("band", ("groups", "sky"), None),
        P("band", ("groups", "sky")),
    )
    out_specs = (P("band", ("groups", "sky"), "epoch"), P("band", ("groups", "sky"), "epoch"))
    return jax.shard_map(
        on_device, mesh=mesh, in_specs=in_specs, out_specs=out_specs, check_vma=False
    )
```

```python
import functools

import jax
import jax.numpy as jnp
from jax import lax
from jax.experimental import pallas as pl
from jax.experimental.pallas import tpu as pltpu
from jax.sharding import PartitionSpec as P


MARGIN = 8
CAPACITY = 2
CLIP_WIDTH = 3.0
TAPS = 6
ROW_BLOCK = 8
LANES = 128
GROUP = 8
UNROLL = 8
LEFT_OVER = 32
NEAR = 4


def lanczos(distance):
    inside = jnp.abs(distance) < 3.0
    return jnp.where(inside, jnp.sinc(distance) * jnp.sinc(distance / 3.0), 0.0)


def tap_weights(fractions):
    gaps = 3.0 - jnp.arange(TAPS, dtype=jnp.float32)
    rounded = lanczos(gaps - fractions[..., None]).astype(jnp.bfloat16)
    return lax.optimization_barrier(rounded).astype(jnp.float32)


def cover(shifts, taps, index, length_in):
    total = jnp.zeros((shifts.shape[0], index.shape[0]), jnp.float32)
    for tap in range(TAPS):
        source = index[None, :] - shifts[:, None] + (tap - 3)
        inside = (source >= 0) & (source < length_in)
        total = total + jnp.where(inside, taps[:, tap][:, None], 0.0)
    return jnp.clip(total, 0.0, 1.0)


def column_kernel(ints, floats, described, pixels, copied, *refs):
    step = pl.program_id(0)
    slots, bands, rows, cols = pixels.shape
    blocks = cols // LANES
    edge = 16
    turn = ints[pl.num_programs(0) * slots]
    outs, (tables, turned) = refs[:-2], refs[-2:]
    parts = len(outs)
    width = cols // parts

    @pl.when(step == 0)
    def _():
        tables[...] = jnp.zeros_like(tables)
        copied[...] = described[...]

    def gap_base(first_row, count, offset):
        k = lax.broadcasted_iota(jnp.int32, (count, LANES), 0) + first_row
        j = lax.broadcasted_iota(jnp.int32, (count, LANES), 1)
        return j - k + offset

    def one(slot, table, ring):
        at = step * slots + slot
        shift = ints[at]
        weights = [floats[at * TAPS + tap] for tap in range(TAPS)]

        def band_of(base):
            gap = base - shift
            value = jnp.zeros(base.shape, jnp.float32)
            for tap in range(TAPS):
                value = jnp.where(gap == 3 - tap, weights[tap], value)
            return value.astype(jnp.bfloat16)

        diagonal = band_of(gap_base(0, LANES, 0))
        upper = band_of(gap_base(LANES - edge, edge, LANES))
        lower = band_of(gap_base(0, edge, -LANES))
        for block in range(blocks):
            low, high = block * LANES, (block + 1) * LANES
            table[low:high, low:high] = diagonal
            if block + 1 < blocks:
                table[high - edge : high, high : high + LANES] = upper
                table[high : high + edge, low:high] = lower
        source = pixels[slot].reshape(bands * rows, cols)
        warped = jnp.dot(source, table[...], preferred_element_type=jnp.float32)
        warped = warped.astype(ring.dtype)
        for part in range(parts):
            for band in range(bands):
                piece = warped[band * rows : (band + 1) * rows, part * width : (part + 1) * width]
                ring[part, :, band * width : (band + 1) * width] = piece
        for ahead in range(parts):
            outs[ahead][slot] = ring[lax.rem(turn + ahead, parts)]

    def pair(index, carry):
        for half in range(2):
            one(index * 2 + half, tables.at[half], turned.at[half])
        return carry

    lax.fori_loop(0, slots // 2, pair, 0)


def warp_columns(pixels, shifts, taps, turn, parts, described):
    held, bands, rows, cols = pixels.shape
    width = bands * cols // parts
    return pl.pallas_call(
        column_kernel,
        grid=(held // GROUP,),
        out_shape=[jax.ShapeDtypeStruct(described.shape, described.dtype)]
        + [jax.ShapeDtypeStruct((held, rows, width), jnp.bfloat16)] * parts,
        in_specs=[
            pl.BlockSpec(memory_space=pltpu.SMEM),
            pl.BlockSpec(memory_space=pltpu.SMEM),
            pl.BlockSpec(described.shape, lambda g: (0, 0)),
            pl.BlockSpec((GROUP, bands, rows, cols), lambda g: (g, 0, 0, 0)),
        ],
        out_specs=[pl.BlockSpec(described.shape, lambda g: (0, 0))]
        + [pl.BlockSpec((GROUP, rows, width), lambda g: (g, 0, 0))] * parts,
        scratch_shapes=[
            pltpu.VMEM((2, cols, cols), jnp.bfloat16),
            pltpu.VMEM((2, parts, rows, width), jnp.bfloat16),
        ],
        compiler_params=pltpu.CompilerParams(dimension_semantics=("arbitrary",)),
        cost_estimate=pl.CostEstimate(
            flops=2 * held * bands * rows * cols * cols,
            bytes_accessed=4 * held * bands * rows * cols,
            transcendentals=0,
        ),
        name="columns",
    )(jnp.append(shifts, turn), taps.reshape(-1), described, pixels)


def clip_kernel(parts, turn, expand, template, *refs):
    scalars, vectors, groups = refs[:parts], refs[parts : 2 * parts], refs[2 * parts : 3 * parts]
    out, framed, sums, planes = refs[3 * parts :]
    slots, rows, width = groups[0].shape
    owners = out.shape[0]
    near = template.shape[0]
    bands = width // LANES
    canvas_rows = rows + 2 * MARGIN
    blocks = canvas_rows // ROW_BLOCK
    cells = vectors[0].shape[1] - LEFT_OVER
    at_taps, at_column_taps, at_scales = cells, cells + TAPS, cells + 2 * TAPS
    at_start = at_scales + 3 * bands
    cols = parts * LANES
    ends = framed.shape[0]
    framed[0:MARGIN, :] = jnp.zeros((MARGIN, width), jnp.float32)
    framed[ends - MARGIN : ends, :] = jnp.zeros((MARGIN, width), jnp.float32)

    def fill(owner, carry):
        start = pl.multiple_of(owner * rows + MARGIN, MARGIN)
        first = pl.multiple_of(owner * rows, rows)
        block = template[lax.rem(owner, near), lax.div(owner, near)]
        framed[pl.ds(start, rows), :] = block.astype(jnp.float32)
        sums[pl.ds(first, rows), :] = jnp.zeros((rows, width), jnp.float32)
        return carry

    lax.fori_loop(0, owners, fill, 0)
    sums[ends - 2 * MARGIN : ends, :] = jnp.zeros((2 * MARGIN, width), jnp.float32)

    lane = lax.broadcasted_iota(jnp.int32, (slots, LANES), 1) + turn[0] * LANES
    for group in range(parts):
        described = vectors[group][...]
        column = lane - described[:, at_start + 2 : at_start + 3].astype(jnp.int32)
        covered = jnp.zeros((slots, LANES), jnp.float32)
        for tap in range(TAPS):
            source = column + (tap - 3)
            inside = (source >= 0) & (source < cols)
            weight = described[:, at_column_taps + tap : at_column_taps + tap + 1]
            covered = covered + jnp.where(inside, weight, 0.0)
        covered = jnp.clip(covered, 0.0, 1.0)
        usable = jnp.dot(
            described.astype(jnp.bfloat16), expand[...], preferred_element_type=jnp.float32
        )
        for block in range(blocks):
            lanes = slice(block * LANES, (block + 1) * LANES)
            planes[group * slots : (group + 1) * slots, lanes] = usable[:, lanes] * covered

    i = lax.broadcasted_iota(jnp.int32, (canvas_rows, LANES), 0)
    k = lax.broadcasted_iota(jnp.int32, (canvas_rows, LANES), 1)
    base = i - MARGIN - k
    ones = jnp.ones((rows, LANES), out.dtype)

    def one(group, slot):
        columns, values = groups[group], scalars[group]
        first = pl.multiple_of(values[slot, at_start].astype(jnp.int32), ROW_BLOCK)
        gap = base - values[slot, at_start + 1].astype(jnp.int32)
        table = jnp.zeros(gap.shape, jnp.float32)
        for tap in range(TAPS):
            table = jnp.where(gap == 3 - tap, values[slot, at_taps + tap], table)
        table = table.astype(columns.dtype)[:, :rows]
        source = jnp.concatenate([columns[slot], ones], axis=1)
        warped = jnp.dot(table, source, preferred_element_type=jnp.float32)
        plane = planes[pl.ds(group * slots + slot, 1), :]
        for block in range(blocks):
            low = block * ROW_BLOCK
            where = pl.ds(first + low, ROW_BLOCK)
            row_cover = jnp.clip(warped[low : low + ROW_BLOCK, width:], 0.0, 1.0)
            weight = row_cover * plane[:, block * LANES : (block + 1) * LANES]
            for band in range(bands):
                lanes = slice(band * LANES, (band + 1) * LANES)
                scale = at_scales + 3 * band
                prior = framed[where, lanes]
                pull = (warped[low : low + ROW_BLOCK, lanes] - prior) * values[slot, scale]
                value = prior * values[slot, scale + 1] + jnp.tanh(pull) * values[slot, scale + 2]
                sums[where, lanes] += weight * value

    def several(group, index, carry):
        for part in range(UNROLL):
            one(group, index * UNROLL + part)
        return carry

    for group in range(parts):
        lax.fori_loop(0, slots // UNROLL, functools.partial(several, group), 0)

    def give(owner, carry):
        start = pl.multiple_of(owner * rows + MARGIN, MARGIN)
        out[owner] = sums[pl.ds(start, rows), :].astype(out.dtype)
        return carry

    lax.fori_loop(0, owners, give, 0)


def clip_and_sum(turn, expand, template, described, columns):
    parts = len(columns)
    slots, rows, width = columns[0].shape
    tiles = parts * slots
    owners = template.shape[0] * template.shape[1]
    height = owners * rows + 2 * MARGIN
    scalar = pl.BlockSpec(memory_space=pltpu.SMEM)
    vector = pl.BlockSpec(memory_space=pltpu.VMEM)
    return pl.pallas_call(
        functools.partial(clip_kernel, parts),
        out_shape=jax.ShapeDtypeStruct((owners, rows, width), jnp.bfloat16),
        in_specs=[scalar, vector, vector] + [scalar] * parts + [vector] * (2 * parts),
        out_specs=vector,
        scratch_shapes=[
            pltpu.VMEM((height, width), jnp.float32),
            pltpu.VMEM((height, width), jnp.float32),
            pltpu.VMEM((tiles, expand.shape[1]), jnp.float32),
        ],
        compiler_params=pltpu.CompilerParams(vmem_limit_bytes=32 * 1024 * 1024),
        cost_estimate=pl.CostEstimate(
            flops=30 * tiles * (rows + 2 * MARGIN) * width,
            bytes_accessed=2 * tiles * rows * width,
            transcendentals=tiles * (rows + 2 * MARGIN) * width,
        ),
        name="clip",
    )(turn, expand, template, *described, *described, *columns)


def spread(index, block_count, block):
    which = jnp.arange(block_count, dtype=jnp.int32)[:, None] == (index // block)[None, :]
    return which.astype(jnp.float32)


def summed_on_arrival(parts, axis, groups=None):
    arrived = lax.all_to_all(
        parts, axis, split_axis=0, concat_axis=0, tiled=True, axis_index_groups=groups
    )
    return functools.reduce(jnp.add, [part.astype(jnp.float32) for part in arrived])


def sky_groups():
    count = lax.axis_size("sky")
    near = NEAR if count % NEAR == 0 else 1
    far = count // near
    near_groups = [[f * near + n for n in range(near)] for f in range(far)]
    far_groups = [[f * near + n for f in range(far)] for n in range(near)]
    return near, far, near_groups, far_groups


def sum_over_sky(parts):
    near, far, near_groups, far_groups = sky_groups()
    parts = jnp.swapaxes(parts.reshape((far, near) + parts.shape[1:]), 0, 1)
    parts = summed_on_arrival(parts, "sky", near_groups).astype(jnp.bfloat16)
    return summed_on_arrival(parts, "sky", far_groups)


def gather_over_sky(shard):
    near, far, near_groups, far_groups = sky_groups()

    def to_all(array, count, groups):
        copies = jnp.broadcast_to(array[None], (count,) + array.shape)
        return lax.all_to_all(
            copies, "sky", split_axis=0, concat_axis=0, tiled=True, axis_index_groups=groups
        )

    shard = to_all(shard, far, far_groups)
    return to_all(shard, near, near_groups)


def from_epochs(pieces):
    count = lax.axis_size("epoch")
    arrived = [pieces[0]]
    for ahead in range(1, count):
        route = [(i, (i + ahead) % count) for i in range(count)]
        arrived.append(lax.ppermute(pieces[ahead], "epoch", route))
    return arrived


def on_device(
    slot_pixels,
    slot_tile,
    slot_offset,
    slot_frac,
    slot_sigma,
    clip_mask,
    slot_count,
    template,
    prior_weight,
):
    sky_count = lax.axis_size("sky")
    epoch_count = lax.axis_size("epoch")
    epoch_position = lax.axis_index("epoch")
    held, bands, rows, cols = slot_pixels.shape
    canvas_rows = rows + 2 * MARGIN
    row_blocks, col_blocks = clip_mask.shape[1:]
    cells = row_blocks * col_blocks
    part_width = cols // epoch_count
    high = lax.Precision.HIGHEST

    template_part = lax.dynamic_slice_in_dim(
        template, epoch_position * part_width, part_width, 2
    )
    sent = jnp.swapaxes(template_part, 0, 1).reshape(rows, bands * part_width)
    whole_template = gather_over_sky(sent)

    target = slot_tile[:, 0]
    sigmas = slot_sigma.astype(jnp.float32)
    over = 1.0 / (sigmas * sigmas)
    scale = CLIP_WIDTH * sigmas
    scales = jnp.stack([1.0 / scale, over, scale * over], 2).reshape(held, 3 * bands)
    taps = tap_weights(slot_frac.astype(jnp.float32))
    live = (jnp.arange(held, dtype=jnp.int32) < slot_count[0]).astype(jnp.float32)
    masks = clip_mask.astype(jnp.float32) * live[:, None, None]
    described = jnp.concatenate(
        [
            masks.reshape(held, cells),
            taps[:, 0],
            taps[:, 1],
            scales,
            (target * rows).astype(jnp.float32)[:, None],
            slot_offset.astype(jnp.float32),
        ],
        1,
    )
    described = jnp.pad(described, ((0, 0), (0, cells + LEFT_OVER - described.shape[1])))

    described, *columns = warp_columns(
        slot_pixels, slot_offset[:, 1], taps[:, 1], epoch_position, epoch_count, described
    )
    columns = from_epochs(columns)
    described = from_epochs([described] * epoch_count)

    row_index = jnp.arange(canvas_rows, dtype=jnp.int32) - MARGIN
    col_index = epoch_position * part_width + jnp.arange(part_width, dtype=jnp.int32)
    all_index = jnp.arange(cols, dtype=jnp.int32)
    expand = spread(col_index, col_blocks, cols // col_blocks)
    cell = jnp.arange(cells + LEFT_OVER, dtype=jnp.int32)[:, None, None]
    of_row = cell // col_blocks == jnp.arange(row_blocks, dtype=jnp.int32)[None, :, None]
    of_col = cell % col_blocks == (col_index // (cols // col_blocks))[None, None, :]
    expand_cells = (of_row & of_col).astype(jnp.bfloat16).reshape(cells + LEFT_OVER, -1)

    row_cover = cover(slot_offset[:, 0], taps[:, 0], row_index, rows)
    col_cover = cover(slot_offset[:, 1], taps[:, 1], all_index, cols)
    block_rows = row_cover.reshape(held, row_blocks, canvas_rows // row_blocks).sum(2)
    block_cols = col_cover.reshape(held, col_blocks, cols // col_blocks).sum(2)
    block = jnp.arange(row_blocks, dtype=jnp.int32)[None, :]
    above = (target[:, None] == 0) & (block == 0)
    below = (target[:, None] == sky_count - 1) & (block == row_blocks - 1)
    block_rows = jnp.where(above | below, 0.0, block_rows)
    tile_total = jnp.sum(masks * block_rows[:, :, None] * block_cols[:, None, :], (1, 2))
    band_part = jnp.sum(tile_total[:, None] * over, 0)
    band_part = band_part + jnp.sum(prior_weight, 1) * (cols / epoch_count)

    facts = jnp.concatenate(
        [
            masks.reshape(held, cells),
            slot_offset.astype(jnp.float32),
            slot_frac.astype(jnp.float32),
            sigmas,
        ],
        1,
    )
    earlier = (target[:, None] == target[None, :]) & (
        jnp.arange(held)[None, :] < jnp.arange(held)[:, None]
    )
    position = target * CAPACITY + jnp.sum(earlier.astype(jnp.int32), 1)
    routes = jnp.arange(sky_count * CAPACITY, dtype=jnp.int32)
    chooser = (position[None, :] == routes[:, None]).astype(jnp.float32)
    chosen = jnp.dot(chooser, facts, precision=high)
    totals = jnp.broadcast_to(band_part[None, :], (chosen.shape[0], bands))
    message = jnp.concatenate([chosen, totals], 1)
    message = jnp.pad(message, ((0, 0), (0, LANES - message.shape[1])))
    message = message.reshape(sky_count, CAPACITY, LANES)
    arrived = lax.all_to_all(message, "sky", split_axis=0, concat_axis=0, tiled=True)
    arrived = jnp.concatenate(from_epochs([arrived] * epoch_count), 0)
    band_total = jnp.sum(arrived[:, 0, cells + 4 + bands : cells + 4 + 2 * bands], 0)

    def unpack(table):
        masks = table[:, :cells].reshape(-1, row_blocks, col_blocks)
        shifts = table[:, cells : cells + 2].astype(jnp.int32)
        taps = tap_weights(table[:, cells + 2 : cells + 4])
        sigmas = table[:, cells + 4 : cells + 4 + bands]
        sigmas = jnp.where(sigmas > 0.0, sigmas, 1.0)
        return masks, shifts, taps, sigmas

    own_masks, own_shift, own_taps, own_sigmas = unpack(arrived.reshape(-1, LANES))
    own_over = 1.0 / (own_sigmas * own_sigmas)
    own_rows = cover(own_shift[:, 0], own_taps[:, 0], row_index, rows)
    own_cols = cover(own_shift[:, 1], own_taps[:, 1], col_index, cols)
    own_plane = jnp.einsum("sik,kj->isj", own_masks, expand, precision=high) * own_cols[None]
    left = own_over[:, :, None, None] * own_rows.reshape(-1, 1, row_blocks, ROW_BLOCK)
    weights = jnp.einsum("sbir,isj->birj", left, own_plane, precision=high)
    weights = weights.reshape(bands, canvas_rows, part_width)
    ring = [(i, i + 1) for i in range(sky_count - 1)]
    from_above = lax.ppermute(weights[:, canvas_rows - MARGIN :], "sky", ring)
    from_below = lax.ppermute(weights[:, :MARGIN], "sky", [(j, i) for i, j in ring])
    weight_sum = weights[:, MARGIN : MARGIN + rows]
    weight_sum = weight_sum.at[:, :MARGIN].add(from_above)
    weight_sum = weight_sum.at[:, rows - MARGIN :].add(from_below)

    partial = clip_and_sum(epoch_position[None], expand_cells, whole_template, described, columns)
    flux = sum_over_sky(partial)
    flux_sum = jnp.swapaxes(flux.reshape(rows, bands, part_width), 0, 1)

    prior = prior_weight[:, :, None]
    depth_map = weight_sum + prior
    coadd_image = (flux_sum + prior * template_part.astype(jnp.float32)) / depth_map
    band_mean = band_total / (rows * sky_count * cols)
    depth_norm = (depth_map / band_mean[:, None, None]).astype(jnp.bfloat16)
    return (coadd_image.astype(jnp.bfloat16), depth_norm)


def solution(mesh):
    in_specs = (
        P(("groups", "sky", "epoch"), "band", None, None),
        P(("groups", "sky", "epoch"), None),
        P(("groups", "sky", "epoch"), None),
        P(("groups", "sky", "epoch"), None),
        P(("groups", "sky", "epoch"), "band"),
        P(("groups", "sky", "epoch"), None, None),
        P(("groups", "sky", "epoch")),
        P("band", ("groups", "sky"), None),
        P("band", ("groups", "sky")),
    )
    out_specs = (P("band", ("groups", "sky"), "epoch"), P("band", ("groups", "sky"), "epoch"))
    return jax.shard_map(
        on_device, mesh=mesh, in_specs=in_specs, out_specs=out_specs, check_vma=False
    )
```

```python
import functools

import jax
import jax.numpy as jnp
from jax import lax
from jax.experimental import pallas as pl
from jax.experimental.pallas import tpu as pltpu
from jax.sharding import PartitionSpec as P


MARGIN = 8
CAPACITY = 2
CLIP_WIDTH = 3.0
TAPS = 6
ROW_BLOCK = 8
LANES = 128
GROUP = 8
UNROLL = 12
LAG = 4
LEFT_OVER = 32
NEAR = 4


def lanczos(distance):
    inside = jnp.abs(distance) < 3.0
    return jnp.where(inside, jnp.sinc(distance) * jnp.sinc(distance / 3.0), 0.0)


def tap_weights(fractions):
    gaps = 3.0 - jnp.arange(TAPS, dtype=jnp.float32)
    rounded = lanczos(gaps - fractions[..., None]).astype(jnp.bfloat16)
    return lax.optimization_barrier(rounded).astype(jnp.float32)


def cover(shifts, taps, index, length_in):
    total = jnp.zeros((shifts.shape[0], index.shape[0]), jnp.float32)
    for tap in range(TAPS):
        source = index[None, :] - shifts[:, None] + (tap - 3)
        inside = (source >= 0) & (source < length_in)
        total = total + jnp.where(inside, taps[:, tap][:, None], 0.0)
    return jnp.clip(total, 0.0, 1.0)


def column_kernel(ints, floats, pixels, *refs):
    step = pl.program_id(0)
    slots, bands, rows, cols = pixels.shape
    blocks = cols // LANES
    edge = 16
    turn = ints[pl.num_programs(0) * slots]
    outs, (tables, turned) = refs[:-2], refs[-2:]
    parts = len(outs)
    width = cols // parts

    @pl.when(step == 0)
    def _():
        tables[...] = jnp.zeros_like(tables)

    def gap_base(first_row, count, offset):
        k = lax.broadcasted_iota(jnp.int32, (count, LANES), 0) + first_row
        j = lax.broadcasted_iota(jnp.int32, (count, LANES), 1)
        return j - k + offset

    def one(slot, table, ring):
        at = step * slots + slot
        shift = ints[at]
        weights = [floats[at * TAPS + tap] for tap in range(TAPS)]

        def band_of(base):
            gap = base - shift
            value = jnp.zeros(base.shape, jnp.float32)
            for tap in range(TAPS):
                value = jnp.where(gap == 3 - tap, weights[tap], value)
            return value.astype(jnp.bfloat16)

        diagonal = band_of(gap_base(0, LANES, 0))
        upper = band_of(gap_base(LANES - edge, edge, LANES))
        lower = band_of(gap_base(0, edge, -LANES))
        for block in range(blocks):
            low, high = block * LANES, (block + 1) * LANES
            table[low:high, low:high] = diagonal
            if block + 1 < blocks:
                table[high - edge : high, high : high + LANES] = upper
                table[high : high + edge, low:high] = lower
        source = pixels[slot].reshape(bands * rows, cols)
        warped = jnp.dot(source, table[...], preferred_element_type=jnp.float32)
        warped = warped.astype(ring.dtype)
        for part in range(parts):
            for band in range(bands):
                piece = warped[band * rows : (band + 1) * rows, part * width : (part + 1) * width]
                ring[part, :, band * width : (band + 1) * width] = piece
        for ahead in range(parts):
            outs[ahead][slot] = ring[lax.rem(turn + ahead, parts)]

    lag = tables.shape[0]

    def several(index, carry):
        for part in range(lag):
            one(index * lag + part, tables.at[part], turned.at[part])
        return carry

    lax.fori_loop(0, slots // lag, several, 0)


def warp_columns(pixels, shifts, taps, turn, parts):
    held, bands, rows, cols = pixels.shape
    width = bands * cols // parts
    return pl.pallas_call(
        column_kernel,
        grid=(held // GROUP,),
        out_shape=[jax.ShapeDtypeStruct((held, rows, width), jnp.bfloat16)] * parts,
        in_specs=[
            pl.BlockSpec(memory_space=pltpu.SMEM),
            pl.BlockSpec(memory_space=pltpu.SMEM),
            pl.BlockSpec((GROUP, bands, rows, cols), lambda g: (g, 0, 0, 0)),
        ],
        out_specs=[pl.BlockSpec((GROUP, rows, width), lambda g: (g, 0, 0))] * parts,
        scratch_shapes=[
            pltpu.VMEM((LAG, cols, cols), jnp.bfloat16),
            pltpu.VMEM((LAG, parts, rows, width), jnp.bfloat16),
        ],
        compiler_params=pltpu.CompilerParams(dimension_semantics=("arbitrary",)),
        cost_estimate=pl.CostEstimate(
            flops=2 * held * bands * rows * cols * cols,
            bytes_accessed=4 * held * bands * rows * cols,
            transcendentals=0,
        ),
        name="columns",
    )(jnp.append(shifts, turn), taps.reshape(-1), pixels)


def clip_kernel(parts, near, turn, expand, *refs):
    templates, refs = refs[:near], refs[near:]
    scalars, vectors, groups = refs[:parts], refs[parts : 2 * parts], refs[2 * parts : 3 * parts]
    out, framed, sums, planes = refs[3 * parts :]
    slots, rows, width = groups[0].shape
    owners = out.shape[0]
    bands = width // LANES
    canvas_rows = rows + 2 * MARGIN
    blocks = canvas_rows // ROW_BLOCK
    cells = vectors[0].shape[1] - LEFT_OVER
    at_taps, at_column_taps, at_scales = cells, cells + TAPS, cells + 2 * TAPS
    at_start = at_scales + 3 * bands
    cols = parts * LANES
    ends = framed.shape[0]
    framed[0:MARGIN, :] = jnp.zeros((MARGIN, width), jnp.float32)
    framed[ends - MARGIN : ends, :] = jnp.zeros((MARGIN, width), jnp.float32)

    def fill(far, carry):
        for behind in range(near):
            owner = far * near + lax.rem(turn[1] - behind + near, near)
            start = pl.multiple_of(owner * rows + MARGIN, MARGIN)
            first = pl.multiple_of(owner * rows, rows)
            framed[pl.ds(start, rows), :] = templates[behind][far].astype(jnp.float32)
            sums[pl.ds(first, rows), :] = jnp.zeros((rows, width), jnp.float32)
        return carry

    lax.fori_loop(0, owners // near, fill, 0)
    sums[ends - 2 * MARGIN : ends, :] = jnp.zeros((2 * MARGIN, width), jnp.float32)

    lane = lax.broadcasted_iota(jnp.int32, (slots, LANES), 1) + turn[0] * LANES
    for group in range(parts):
        described = vectors[group][...]
        column = lane - described[:, at_start + 2 : at_start + 3].astype(jnp.int32)
        covered = jnp.zeros((slots, LANES), jnp.float32)
        for tap in range(TAPS):
            source = column + (tap - 3)
            inside = (source >= 0) & (source < cols)
            weight = described[:, at_column_taps + tap : at_column_taps + tap + 1]
            covered = covered + jnp.where(inside, weight, 0.0)
        covered = jnp.clip(covered, 0.0, 1.0)
        usable = jnp.dot(
            described.astype(jnp.bfloat16), expand[...], preferred_element_type=jnp.float32
        )
        for block in range(blocks):
            lanes = slice(block * LANES, (block + 1) * LANES)
            planes[group * slots : (group + 1) * slots, lanes] = usable[:, lanes] * covered

    i = lax.broadcasted_iota(jnp.int32, (canvas_rows, LANES), 0)
    k = lax.broadcasted_iota(jnp.int32, (canvas_rows, LANES), 1)
    base = i - MARGIN - k
    ones = jnp.ones((rows, LANES), out.dtype)

    def one(group, slot):
        columns, values = groups[group], scalars[group]
        first = pl.multiple_of(values[slot, at_start].astype(jnp.int32), ROW_BLOCK)
        gap = base - values[slot, at_start + 1].astype(jnp.int32)
        table = jnp.zeros(gap.shape, jnp.float32)
        for tap in range(TAPS):
            table = jnp.where(gap == 3 - tap, values[slot, at_taps + tap], table)
        table = table.astype(columns.dtype)[:, :rows]
        source = jnp.concatenate([columns[slot], ones], axis=1)
        warped = jnp.dot(table, source, preferred_element_type=jnp.float32)
        plane = planes[pl.ds(group * slots + slot, 1), :]
        for block in range(blocks):
            low = block * ROW_BLOCK
            where = pl.ds(first + low, ROW_BLOCK)
            row_cover = jnp.clip(warped[low : low + ROW_BLOCK, width:], 0.0, 1.0)
            weight = row_cover * plane[:, block * LANES : (block + 1) * LANES]
            for band in range(bands):
                lanes = slice(band * LANES, (band + 1) * LANES)
                scale = at_scales + 3 * band
                prior = framed[where, lanes]
                pull = (warped[low : low + ROW_BLOCK, lanes] - prior) * values[slot, scale]
                value = prior * values[slot, scale + 1] + jnp.tanh(pull) * values[slot, scale + 2]
                sums[where, lanes] += weight * value

    def several(group, index, carry):
        for part in range(UNROLL):
            one(group, index * UNROLL + part)
        return carry

    for group in range(parts):
        lax.fori_loop(0, slots // UNROLL, functools.partial(several, group), 0)

    def give(owner, carry):
        start = pl.multiple_of(owner * rows + MARGIN, MARGIN)
        out[owner] = sums[pl.ds(start, rows), :].astype(out.dtype)
        return carry

    lax.fori_loop(0, owners, give, 0)


def clip_and_sum(turn, expand, templates, described, columns):
    parts, near = len(columns), len(templates)
    slots, rows, width = columns[0].shape
    tiles = parts * slots
    owners = near * templates[0].shape[0]
    height = owners * rows + 2 * MARGIN
    scalar = pl.BlockSpec(memory_space=pltpu.SMEM)
    vector = pl.BlockSpec(memory_space=pltpu.VMEM)
    return pl.pallas_call(
        functools.partial(clip_kernel, parts, near),
        out_shape=jax.ShapeDtypeStruct((owners, rows, width), jnp.bfloat16),
        in_specs=[scalar] + [vector] * (1 + near) + [scalar] * parts + [vector] * (2 * parts),
        out_specs=vector,
        scratch_shapes=[
            pltpu.VMEM((height, width), jnp.float32),
            pltpu.VMEM((height, width), jnp.float32),
            pltpu.VMEM((tiles, expand.shape[1]), jnp.float32),
        ],
        compiler_params=pltpu.CompilerParams(vmem_limit_bytes=32 * 1024 * 1024),
        cost_estimate=pl.CostEstimate(
            flops=30 * tiles * (rows + 2 * MARGIN) * width,
            bytes_accessed=2 * tiles * rows * width,
            transcendentals=tiles * (rows + 2 * MARGIN) * width,
        ),
        name="clip",
    )(turn, expand, *templates, *described, *described, *columns)


def spread(index, block_count, block):
    which = jnp.arange(block_count, dtype=jnp.int32)[:, None] == (index // block)[None, :]
    return which.astype(jnp.float32)


def summed_on_arrival(parts, axis, groups=None):
    arrived = lax.all_to_all(
        parts, axis, split_axis=0, concat_axis=0, tiled=True, axis_index_groups=groups
    )
    return functools.reduce(jnp.add, [part.astype(jnp.float32) for part in arrived])


def sky_groups():
    count = lax.axis_size("sky")
    near = NEAR if count % NEAR == 0 else 1
    far = count // near
    near_groups = [[f * near + n for n in range(near)] for f in range(far)]
    far_groups = [[f * near + n for f in range(far)] for n in range(near)]
    return near, far, near_groups, far_groups


def sum_over_sky(parts):
    near, far, near_groups, far_groups = sky_groups()
    parts = jnp.swapaxes(parts.reshape((far, near) + parts.shape[1:]), 0, 1)
    parts = summed_on_arrival(parts, "sky", near_groups).astype(jnp.bfloat16)
    return summed_on_arrival(parts, "sky", far_groups)


def gather_over_sky(shard):
    near, far, near_groups, far_groups = sky_groups()
    copies = jnp.broadcast_to(shard[None], (far,) + shard.shape)
    shards = lax.all_to_all(
        copies, "sky", split_axis=0, concat_axis=0, tiled=True, axis_index_groups=far_groups
    )
    arrived = [shards]
    for ahead in range(1, near):
        route = [(g[i], g[(i + ahead) % near]) for g in near_groups for i in range(near)]
        arrived.append(lax.ppermute(shards, "sky", route))
    return arrived


def from_epochs(pieces):
    count = lax.axis_size("epoch")
    arrived = [pieces[0]]
    for ahead in range(1, count):
        route = [(i, (i + ahead) % count) for i in range(count)]
        arrived.append(lax.ppermute(pieces[ahead], "epoch", route))
    return arrived


def on_device(
    slot_pixels,
    slot_tile,
    slot_offset,
    slot_frac,
    slot_sigma,
    clip_mask,
    slot_count,
    template,
    prior_weight,
):
    sky_count = lax.axis_size("sky")
    epoch_count = lax.axis_size("epoch")
    epoch_position = lax.axis_index("epoch")
    held, bands, rows, cols = slot_pixels.shape
    canvas_rows = rows + 2 * MARGIN
    row_blocks, col_blocks = clip_mask.shape[1:]
    cells = row_blocks * col_blocks
    part_width = cols // epoch_count
    high = lax.Precision.HIGHEST

    template_part = lax.dynamic_slice_in_dim(
        template, epoch_position * part_width, part_width, 2
    )
    sent = jnp.swapaxes(template_part, 0, 1).reshape(rows, bands * part_width)
    templates = gather_over_sky(sent)

    target = slot_tile[:, 0]
    sigmas = slot_sigma.astype(jnp.float32)
    over = 1.0 / (sigmas * sigmas)
    scale = CLIP_WIDTH * sigmas
    scales = jnp.stack([1.0 / scale, over, scale * over], 2).reshape(held, 3 * bands)
    taps = tap_weights(slot_frac.astype(jnp.float32))
    live = (jnp.arange(held, dtype=jnp.int32) < slot_count[0]).astype(jnp.float32)
    masks = clip_mask.astype(jnp.float32) * live[:, None, None]
    described = jnp.concatenate(
        [
            masks.reshape(held, cells),
            taps[:, 0],
            taps[:, 1],
            scales,
            (target * rows).astype(jnp.float32)[:, None],
            slot_offset.astype(jnp.float32),
        ],
        1,
    )
    described = jnp.pad(described, ((0, 0), (0, cells + LEFT_OVER - described.shape[1])))

    columns = warp_columns(slot_pixels, slot_offset[:, 1], taps[:, 1], epoch_position, epoch_count)
    columns = from_epochs(columns)
    described = from_epochs([described] * epoch_count)

    row_index = jnp.arange(canvas_rows, dtype=jnp.int32) - MARGIN
    col_index = epoch_position * part_width + jnp.arange(part_width, dtype=jnp.int32)
    all_index = jnp.arange(cols, dtype=jnp.int32)
    expand = spread(col_index, col_blocks, cols // col_blocks)
    cell = jnp.arange(cells + LEFT_OVER, dtype=jnp.int32)[:, None, None]
    of_row = cell // col_blocks == jnp.arange(row_blocks, dtype=jnp.int32)[None, :, None]
    of_col = cell % col_blocks == (col_index // (cols // col_blocks))[None, None, :]
    expand_cells = (of_row & of_col).astype(jnp.bfloat16).reshape(cells + LEFT_OVER, -1)

    row_cover = cover(slot_offset[:, 0], taps[:, 0], row_index, rows)
    col_cover = cover(slot_offset[:, 1], taps[:, 1], all_index, cols)
    block_rows = row_cover.reshape(held, row_blocks, canvas_rows // row_blocks).sum(2)
    block_cols = col_cover.reshape(held, col_blocks, cols // col_blocks).sum(2)
    block = jnp.arange(row_blocks, dtype=jnp.int32)[None, :]
    above = (target[:, None] == 0) & (block == 0)
    below = (target[:, None] == sky_count - 1) & (block == row_blocks - 1)
    block_rows = jnp.where(above | below, 0.0, block_rows)
    tile_total = jnp.sum(masks * block_rows[:, :, None] * block_cols[:, None, :], (1, 2))
    band_part = jnp.sum(tile_total[:, None] * over, 0)
    band_part = band_part + jnp.sum(prior_weight, 1) * (cols / epoch_count)

    facts = jnp.concatenate(
        [
            masks.reshape(held, cells),
            slot_offset.astype(jnp.float32),
            slot_frac.astype(jnp.float32),
            sigmas,
        ],
        1,
    )
    earlier = (target[:, None] == target[None, :]) & (
        jnp.arange(held)[None, :] < jnp.arange(held)[:, None]
    )
    position = target * CAPACITY + jnp.sum(earlier.astype(jnp.int32), 1)
    routes = jnp.arange(sky_count * CAPACITY, dtype=jnp.int32)
    chooser = (position[None, :] == routes[:, None]).astype(jnp.float32)
    chosen = jnp.dot(chooser, facts, precision=high)
    totals = jnp.broadcast_to(band_part[None, :], (chosen.shape[0], bands))
    message = jnp.concatenate([chosen, totals], 1)
    message = jnp.pad(message, ((0, 0), (0, LANES - message.shape[1])))
    message = message.reshape(sky_count, CAPACITY, LANES)
    arrived = lax.all_to_all(message, "sky", split_axis=0, concat_axis=0, tiled=True)
    arrived = jnp.concatenate(from_epochs([arrived] * epoch_count), 0)
    band_total = jnp.sum(arrived[:, 0, cells + 4 + bands : cells + 4 + 2 * bands], 0)

    def unpack(table):
        masks = table[:, :cells].reshape(-1, row_blocks, col_blocks)
        shifts = table[:, cells : cells + 2].astype(jnp.int32)
        taps = tap_weights(table[:, cells + 2 : cells + 4])
        sigmas = table[:, cells + 4 : cells + 4 + bands]
        sigmas = jnp.where(sigmas > 0.0, sigmas, 1.0)
        return masks, shifts, taps, sigmas

    own_masks, own_shift, own_taps, own_sigmas = unpack(arrived.reshape(-1, LANES))
    own_over = 1.0 / (own_sigmas * own_sigmas)
    own_rows = cover(own_shift[:, 0], own_taps[:, 0], row_index, rows)
    own_cols = cover(own_shift[:, 1], own_taps[:, 1], col_index, cols)
    own_plane = jnp.einsum("sik,kj->isj", own_masks, expand, precision=high) * own_cols[None]
    left = own_over[:, :, None, None] * own_rows.reshape(-1, 1, row_blocks, ROW_BLOCK)
    weights = jnp.einsum("sbir,isj->birj", left, own_plane, precision=high)
    weights = weights.reshape(bands, canvas_rows, part_width)
    ring = [(i, i + 1) for i in range(sky_count - 1)]
    from_above = lax.ppermute(weights[:, canvas_rows - MARGIN :], "sky", ring)
    from_below = lax.ppermute(weights[:, :MARGIN], "sky", [(j, i) for i, j in ring])
    weight_sum = weights[:, MARGIN : MARGIN + rows]
    weight_sum = weight_sum.at[:, :MARGIN].add(from_above)
    weight_sum = weight_sum.at[:, rows - MARGIN :].add(from_below)

    turn = jnp.stack([epoch_position, lax.axis_index("sky") % len(templates)])
    partial = clip_and_sum(turn, expand_cells, templates, described, columns)
    flux = sum_over_sky(partial)
    flux_sum = jnp.swapaxes(flux.reshape(rows, bands, part_width), 0, 1)

    prior = prior_weight[:, :, None]
    depth_map = weight_sum + prior
    coadd_image = (flux_sum + prior * template_part.astype(jnp.float32)) / depth_map
    band_mean = band_total / (rows * sky_count * cols)
    depth_norm = (depth_map / band_mean[:, None, None]).astype(jnp.bfloat16)
    return (coadd_image.astype(jnp.bfloat16), depth_norm)


def solution(mesh):
    in_specs = (
        P(("groups", "sky", "epoch"), "band", None, None),
        P(("groups", "sky", "epoch"), None),
        P(("groups", "sky", "epoch"), None),
        P(("groups", "sky", "epoch"), None),
        P(("groups", "sky", "epoch"), "band"),
        P(("groups", "sky", "epoch"), None, None),
        P(("groups", "sky", "epoch")),
        P("band", ("groups", "sky"), None),
        P("band", ("groups", "sky")),
    )
    out_specs = (P("band", ("groups", "sky"), "epoch"), P("band", ("groups", "sky"), "epoch"))
    return jax.shard_map(
        on_device, mesh=mesh, in_specs=in_specs, out_specs=out_specs, check_vma=False
    )
```

```python
import functools

import jax
import jax.numpy as jnp
from jax import lax
from jax.experimental import pallas as pl
from jax.experimental.pallas import tpu as pltpu
from jax.sharding import PartitionSpec as P


MARGIN = 8
CAPACITY = 2
CLIP_WIDTH = 3.0
TAPS = 6
ROW_BLOCK = 8
LANES = 128
GROUP = 8
UNROLL = 12
LAG = 4
LEFT_OVER = 32
NEAR = 4


def lanczos(distance):
    inside = jnp.abs(distance) < 3.0
    return jnp.where(inside, jnp.sinc(distance) * jnp.sinc(distance / 3.0), 0.0)


def tap_weights(fractions):
    gaps = 3.0 - jnp.arange(TAPS, dtype=jnp.float32)
    rounded = lanczos(gaps - fractions[..., None]).astype(jnp.bfloat16)
    return lax.optimization_barrier(rounded).astype(jnp.float32)


def cover(shifts, taps, index, length_in):
    total = jnp.zeros((shifts.shape[0], index.shape[0]), jnp.float32)
    for tap in range(TAPS):
        source = index[None, :] - shifts[:, None] + (tap - 3)
        inside = (source >= 0) & (source < length_in)
        total = total + jnp.where(inside, taps[:, tap][:, None], 0.0)
    return jnp.clip(total, 0.0, 1.0)


def column_kernel(ints, floats, facts, pixels, *refs):
    step = pl.program_id(0)
    slots, bands, rows, cols = pixels.shape
    blocks = cols // LANES
    edge = 16
    turn = ints[pl.num_programs(0) * slots]
    outs, (tables, turned) = refs[:-2], refs[-2:]
    parts = len(outs)
    width = cols // parts

    @pl.when(step == 0)
    def _():
        tables[...] = jnp.zeros_like(tables)
        for piece in outs:
            piece[piece.shape[0] - 1, 0 : facts.shape[0], :] = facts[...]
            piece[piece.shape[0] - 1, facts.shape[0] :, :] = jnp.zeros_like(facts)

    def gap_base(first_row, count, offset):
        k = lax.broadcasted_iota(jnp.int32, (count, LANES), 0) + first_row
        j = lax.broadcasted_iota(jnp.int32, (count, LANES), 1)
        return j - k + offset

    def one(slot, table, ring):
        at = step * slots + slot
        shift = ints[at]
        weights = [floats[at * TAPS + tap] for tap in range(TAPS)]

        def band_of(base):
            gap = base - shift
            value = jnp.zeros(base.shape, jnp.float32)
            for tap in range(TAPS):
                value = jnp.where(gap == 3 - tap, weights[tap], value)
            return value.astype(jnp.bfloat16)

        diagonal = band_of(gap_base(0, LANES, 0))
        upper = band_of(gap_base(LANES - edge, edge, LANES))
        lower = band_of(gap_base(0, edge, -LANES))
        for block in range(blocks):
            low, high = block * LANES, (block + 1) * LANES
            table[low:high, low:high] = diagonal
            if block + 1 < blocks:
                table[high - edge : high, high : high + LANES] = upper
                table[high : high + edge, low:high] = lower
        source = pixels[slot].reshape(bands * rows, cols)
        warped = jnp.dot(source, table[...], preferred_element_type=jnp.float32)
        warped = warped.astype(ring.dtype)
        for part in range(parts):
            for band in range(bands):
                piece = warped[band * rows : (band + 1) * rows, part * width : (part + 1) * width]
                ring[part, :, band * width : (band + 1) * width] = piece
        for ahead in range(parts):
            outs[ahead][at] = ring[lax.rem(turn + ahead, parts)]

    lag = tables.shape[0]

    def several(index, carry):
        for part in range(lag):
            one(index * lag + part, tables.at[part], turned.at[part])
        return carry

    lax.fori_loop(0, slots // lag, several, 0)


def warp_columns(pixels, shifts, taps, turn, parts, facts):
    held, bands, rows, cols = pixels.shape
    width = bands * cols // parts
    return pl.pallas_call(
        column_kernel,
        grid=(held // GROUP,),
        out_shape=[jax.ShapeDtypeStruct((held + 1, rows, width), jnp.bfloat16)] * parts,
        in_specs=[
            pl.BlockSpec(memory_space=pltpu.SMEM),
            pl.BlockSpec(memory_space=pltpu.SMEM),
            pl.BlockSpec(facts.shape, lambda g: (0, 0)),
            pl.BlockSpec((GROUP, bands, rows, cols), lambda g: (g, 0, 0, 0)),
        ],
        out_specs=[pl.BlockSpec((held + 1, rows, width), lambda g: (0, 0, 0))] * parts,
        scratch_shapes=[
            pltpu.VMEM((LAG, cols, cols), jnp.bfloat16),
            pltpu.VMEM((LAG, parts, rows, width), jnp.bfloat16),
        ],
        compiler_params=pltpu.CompilerParams(dimension_semantics=("arbitrary",)),
        cost_estimate=pl.CostEstimate(
            flops=2 * held * bands * rows * cols * cols,
            bytes_accessed=4 * held * bands * rows * cols,
            transcendentals=0,
        ),
        name="columns",
    )(jnp.append(shifts, turn), taps.reshape(-1), facts, pixels)


def clip_kernel(parts, near, turn, expand, *refs):
    templates, refs = refs[:near], refs[near:]
    groups = refs[:parts]
    out, framed, sums, planes, vectors, scalars, arrival = refs[parts:]
    slots, rows, width = groups[0].shape
    slots -= 1
    owners = out.shape[0]
    bands = width // LANES
    canvas_rows = rows + 2 * MARGIN
    blocks = canvas_rows // ROW_BLOCK
    cells = vectors.shape[1] - LEFT_OVER
    at_taps, at_column_taps, at_scales = cells, cells + TAPS, cells + 2 * TAPS
    at_start = at_scales + 3 * bands
    at_sigmas = at_start + 3
    cols = parts * LANES

    share = slots // bands
    place = lax.broadcasted_iota(jnp.int32, (share, LANES), 1)
    for group in range(parts):
        for third in range(bands):
            lanes = slice(third * LANES, (third + 1) * LANES)
            facts = groups[group][slots, 0:share, lanes].astype(jnp.float32)
            for band in range(bands):
                sigma = facts[:, at_sigmas + band : at_sigmas + band + 1]
                scale = CLIP_WIDTH * sigma
                over = 1.0 / (sigma * sigma)
                for number, value in enumerate((1.0 / scale, over, scale * over)):
                    facts = jnp.where(place == at_scales + 3 * band + number, value, facts)
            low = group * slots + third * share
            vectors[low : low + share, :] = facts
    ends = framed.shape[0]
    framed[0:MARGIN, :] = jnp.zeros((MARGIN, width), jnp.float32)
    framed[ends - MARGIN : ends, :] = jnp.zeros((MARGIN, width), jnp.float32)

    def fill(far, carry):
        for behind in range(near):
            owner = far * near + lax.rem(turn[1] - behind + near, near)
            start = pl.multiple_of(owner * rows + MARGIN, MARGIN)
            first = pl.multiple_of(owner * rows, rows)
            framed[pl.ds(start, rows), :] = templates[behind][far].astype(jnp.float32)
            sums[pl.ds(first, rows), :] = jnp.zeros((rows, width), jnp.float32)
        return carry

    lax.fori_loop(0, owners // near, fill, 0)
    sums[ends - 2 * MARGIN : ends, :] = jnp.zeros((2 * MARGIN, width), jnp.float32)

    lane = lax.broadcasted_iota(jnp.int32, (slots, LANES), 1) + turn[0] * LANES
    for group in range(parts):
        described = vectors[group * slots : (group + 1) * slots, :]
        column = lane - described[:, at_start + 2 : at_start + 3].astype(jnp.int32)
        covered = jnp.zeros((slots, LANES), jnp.float32)
        for tap in range(TAPS):
            source = column + (tap - 3)
            inside = (source >= 0) & (source < cols)
            weight = described[:, at_column_taps + tap : at_column_taps + tap + 1]
            covered = covered + jnp.where(inside, weight, 0.0)
        covered = jnp.clip(covered, 0.0, 1.0)
        usable = jnp.dot(
            described.astype(jnp.bfloat16), expand[...], preferred_element_type=jnp.float32
        )
        for block in range(blocks):
            lanes = slice(block * LANES, (block + 1) * LANES)
            planes[group * slots : (group + 1) * slots, lanes] = usable[:, lanes] * covered

    copy = pltpu.make_async_copy(vectors, scalars, arrival)
    copy.start()
    copy.wait()

    i = lax.broadcasted_iota(jnp.int32, (canvas_rows, LANES), 0)
    k = lax.broadcasted_iota(jnp.int32, (canvas_rows, LANES), 1)
    base = i - MARGIN - k
    ones = jnp.ones((rows, LANES), out.dtype)

    def one(group, slot):
        columns, at = groups[group], group * slots + slot
        first = pl.multiple_of(scalars[at, at_start].astype(jnp.int32), ROW_BLOCK)
        gap = base - scalars[at, at_start + 1].astype(jnp.int32)
        table = jnp.zeros(gap.shape, jnp.float32)
        for tap in range(TAPS):
            table = jnp.where(gap == 3 - tap, scalars[at, at_taps + tap], table)
        table = table.astype(columns.dtype)[:, :rows]
        source = jnp.concatenate([columns[slot], ones], axis=1)
        warped = jnp.dot(table, source, preferred_element_type=jnp.float32)
        plane = planes[pl.ds(at, 1), :]
        for block in range(blocks):
            low = block * ROW_BLOCK
            where = pl.ds(first + low, ROW_BLOCK)
            row_cover = jnp.clip(warped[low : low + ROW_BLOCK, width:], 0.0, 1.0)
            weight = row_cover * plane[:, block * LANES : (block + 1) * LANES]
            for band in range(bands):
                lanes = slice(band * LANES, (band + 1) * LANES)
                scale = at_scales + 3 * band
                prior = framed[where, lanes]
                pull = (warped[low : low + ROW_BLOCK, lanes] - prior) * scalars[at, scale]
                value = prior * scalars[at, scale + 1] + jnp.tanh(pull) * scalars[at, scale + 2]
                sums[where, lanes] += weight * value

    def several(group, index, carry):
        for part in range(UNROLL):
            one(group, index * UNROLL + part)
        return carry

    for group in range(parts):
        lax.fori_loop(0, slots // UNROLL, functools.partial(several, group), 0)

    def give(owner, carry):
        start = pl.multiple_of(owner * rows + MARGIN, MARGIN)
        out[owner] = sums[pl.ds(start, rows), :].astype(out.dtype)
        return carry

    lax.fori_loop(0, owners, give, 0)


def clip_and_sum(turn, expand, templates, columns):
    parts, near = len(columns), len(templates)
    slots, rows, width = columns[0].shape
    tiles = parts * (slots - 1)
    owners = near * templates[0].shape[0]
    height = owners * rows + 2 * MARGIN
    scalar = pl.BlockSpec(memory_space=pltpu.SMEM)
    vector = pl.BlockSpec(memory_space=pltpu.VMEM)
    return pl.pallas_call(
        functools.partial(clip_kernel, parts, near),
        out_shape=jax.ShapeDtypeStruct((owners, rows, width), jnp.bfloat16),
        in_specs=[scalar] + [vector] * (1 + near + parts),
        out_specs=vector,
        scratch_shapes=[
            pltpu.VMEM((height, width), jnp.float32),
            pltpu.VMEM((height, width), jnp.float32),
            pltpu.VMEM((tiles, expand.shape[1]), jnp.float32),
            pltpu.VMEM((tiles, expand.shape[0]), jnp.float32),
            pltpu.SMEM((tiles, expand.shape[0]), jnp.float32),
            pltpu.SemaphoreType.DMA,
        ],
        compiler_params=pltpu.CompilerParams(vmem_limit_bytes=32 * 1024 * 1024),
        cost_estimate=pl.CostEstimate(
            flops=30 * tiles * (rows + 2 * MARGIN) * width,
            bytes_accessed=2 * tiles * rows * width,
            transcendentals=tiles * (rows + 2 * MARGIN) * width,
        ),
        name="clip",
    )(turn, expand, *templates, *columns)


def spread(index, block_count, block):
    which = jnp.arange(block_count, dtype=jnp.int32)[:, None] == (index // block)[None, :]
    return which.astype(jnp.float32)


def summed_on_arrival(parts, axis, groups=None):
    arrived = lax.all_to_all(
        parts, axis, split_axis=0, concat_axis=0, tiled=True, axis_index_groups=groups
    )
    return functools.reduce(jnp.add, [part.astype(jnp.float32) for part in arrived])


def sky_groups():
    count = lax.axis_size("sky")
    near = NEAR if count % NEAR == 0 else 1
    far = count // near
    near_groups = [[f * near + n for n in range(near)] for f in range(far)]
    far_groups = [[f * near + n for f in range(far)] for n in range(near)]
    return near, far, near_groups, far_groups


def sum_over_sky(parts):
    near, far, near_groups, far_groups = sky_groups()
    parts = jnp.swapaxes(parts.reshape((far, near) + parts.shape[1:]), 0, 1)
    parts = summed_on_arrival(parts, "sky", near_groups).astype(jnp.bfloat16)
    return summed_on_arrival(parts, "sky", far_groups)


def gather_over_sky(shard):
    near, far, near_groups, far_groups = sky_groups()
    copies = jnp.broadcast_to(shard[None], (far,) + shard.shape)
    shards = lax.all_to_all(
        copies, "sky", split_axis=0, concat_axis=0, tiled=True, axis_index_groups=far_groups
    )
    arrived = [shards]
    for ahead in range(1, near):
        route = [(g[i], g[(i + ahead) % near]) for g in near_groups for i in range(near)]
        arrived.append(lax.ppermute(shards, "sky", route))
    return arrived


def from_epochs(pieces):
    count = lax.axis_size("epoch")
    arrived = [pieces[0]]
    for ahead in range(1, count):
        route = [(i, (i + ahead) % count) for i in range(count)]
        arrived.append(lax.ppermute(pieces[ahead], "epoch", route))
    return arrived


def on_device(
    slot_pixels,
    slot_tile,
    slot_offset,
    slot_frac,
    slot_sigma,
    clip_mask,
    slot_count,
    template,
    prior_weight,
):
    sky_count = lax.axis_size("sky")
    epoch_count = lax.axis_size("epoch")
    epoch_position = lax.axis_index("epoch")
    held, bands, rows, cols = slot_pixels.shape
    canvas_rows = rows + 2 * MARGIN
    row_blocks, col_blocks = clip_mask.shape[1:]
    cells = row_blocks * col_blocks
    part_width = cols // epoch_count
    high = lax.Precision.HIGHEST

    template_part = lax.dynamic_slice_in_dim(
        template, epoch_position * part_width, part_width, 2
    )
    sent = jnp.swapaxes(template_part, 0, 1).reshape(rows, bands * part_width)
    templates = gather_over_sky(sent)

    target = slot_tile[:, 0]
    sigmas = slot_sigma.astype(jnp.float32)
    over = 1.0 / (sigmas * sigmas)
    taps = tap_weights(slot_frac.astype(jnp.float32))
    live = (jnp.arange(held, dtype=jnp.int32) < slot_count[0]).astype(jnp.float32)
    masks = clip_mask.astype(jnp.float32) * live[:, None, None]
    described = jnp.concatenate(
        [
            masks.reshape(held, cells),
            taps[:, 0],
            taps[:, 1],
            jnp.zeros((held, 3 * bands), jnp.float32),
            (target * rows).astype(jnp.float32)[:, None],
            slot_offset.astype(jnp.float32),
            sigmas,
        ],
        1,
    )
    described = jnp.pad(described, ((0, 0), (0, cells + LEFT_OVER - described.shape[1])))
    described = described.astype(jnp.bfloat16).reshape(bands, held // bands, -1)
    described = jnp.swapaxes(described, 0, 1).reshape(held // bands, -1)

    columns = warp_columns(
        slot_pixels, slot_offset[:, 1], taps[:, 1], epoch_position, epoch_count, described
    )
    columns = from_epochs(columns)

    row_index = jnp.arange(canvas_rows, dtype=jnp.int32) - MARGIN
    col_index = epoch_position * part_width + jnp.arange(part_width, dtype=jnp.int32)
    all_index = jnp.arange(cols, dtype=jnp.int32)
    expand = spread(col_index, col_blocks, cols // col_blocks)
    cell = jnp.arange(cells + LEFT_OVER, dtype=jnp.int32)[:, None, None]
    of_row = cell // col_blocks == jnp.arange(row_blocks, dtype=jnp.int32)[None, :, None]
    of_col = cell % col_blocks == (col_index // (cols // col_blocks))[None, None, :]
    expand_cells = (of_row & of_col).astype(jnp.bfloat16).reshape(cells + LEFT_OVER, -1)

    row_cover = cover(slot_offset[:, 0], taps[:, 0], row_index, rows)
    col_cover = cover(slot_offset[:, 1], taps[:, 1], all_index, cols)
    block_rows = row_cover.reshape(held, row_blocks, canvas_rows // row_blocks).sum(2)
    block_cols = col_cover.reshape(held, col_blocks, cols // col_blocks).sum(2)
    block = jnp.arange(row_blocks, dtype=jnp.int32)[None, :]
    above = (target[:, None] == 0) & (block == 0)
    below = (target[:, None] == sky_count - 1) & (block == row_blocks - 1)
    block_rows = jnp.where(above | below, 0.0, block_rows)
    tile_total = jnp.sum(masks * block_rows[:, :, None] * block_cols[:, None, :], (1, 2))
    band_part = jnp.sum(tile_total[:, None] * over, 0)
    band_part = band_part + jnp.sum(prior_weight, 1) * (cols / epoch_count)

    facts = jnp.concatenate(
        [
            masks.reshape(held, cells),
            slot_offset.astype(jnp.float32),
            slot_frac.astype(jnp.float32),
            sigmas,
        ],
        1,
    )
    earlier = (target[:, None] == target[None, :]) & (
        jnp.arange(held)[None, :] < jnp.arange(held)[:, None]
    )
    position = target * CAPACITY + jnp.sum(earlier.astype(jnp.int32), 1)
    routes = jnp.arange(sky_count * CAPACITY, dtype=jnp.int32)
    chooser = (position[None, :] == routes[:, None]).astype(jnp.float32)
    chosen = jnp.dot(chooser, facts, precision=high)
    totals = jnp.broadcast_to(band_part[None, :], (chosen.shape[0], bands))
    message = jnp.concatenate([chosen, totals], 1)
    message = jnp.pad(message, ((0, 0), (0, LANES - message.shape[1])))
    message = message.reshape(sky_count, CAPACITY, LANES)
    arrived = lax.all_to_all(message, "sky", split_axis=0, concat_axis=0, tiled=True)
    arrived = jnp.concatenate(from_epochs([arrived] * epoch_count), 0)
    band_total = jnp.sum(arrived[:, 0, cells + 4 + bands : cells + 4 + 2 * bands], 0)

    def unpack(table):
        masks = table[:, :cells].reshape(-1, row_blocks, col_blocks)
        shifts = table[:, cells : cells + 2].astype(jnp.int32)
        taps = tap_weights(table[:, cells + 2 : cells + 4])
        sigmas = table[:, cells + 4 : cells + 4 + bands]
        sigmas = jnp.where(sigmas > 0.0, sigmas, 1.0)
        return masks, shifts, taps, sigmas

    own_masks, own_shift, own_taps, own_sigmas = unpack(arrived.reshape(-1, LANES))
    own_over = 1.0 / (own_sigmas * own_sigmas)
    own_rows = cover(own_shift[:, 0], own_taps[:, 0], row_index, rows)
    own_cols = cover(own_shift[:, 1], own_taps[:, 1], col_index, cols)
    own_plane = jnp.einsum("sik,kj->isj", own_masks, expand, precision=high) * own_cols[None]
    left = own_over[:, :, None, None] * own_rows.reshape(-1, 1, row_blocks, ROW_BLOCK)
    weights = jnp.einsum("sbir,isj->birj", left, own_plane, precision=high)
    weights = weights.reshape(bands, canvas_rows, part_width)
    ring = [(i, i + 1) for i in range(sky_count - 1)]
    from_above = lax.ppermute(weights[:, canvas_rows - MARGIN :], "sky", ring)
    from_below = lax.ppermute(weights[:, :MARGIN], "sky", [(j, i) for i, j in ring])
    weight_sum = weights[:, MARGIN : MARGIN + rows]
    weight_sum = weight_sum.at[:, :MARGIN].add(from_above)
    weight_sum = weight_sum.at[:, rows - MARGIN :].add(from_below)

    turn = jnp.stack([epoch_position, lax.axis_index("sky") % len(templates)])
    partial = clip_and_sum(turn, expand_cells, templates, columns)
    flux = sum_over_sky(partial)
    flux_sum = jnp.swapaxes(flux.reshape(rows, bands, part_width), 0, 1)

    prior = prior_weight[:, :, None]
    depth_map = weight_sum + prior
    coadd_image = (flux_sum + prior * template_part.astype(jnp.float32)) / depth_map
    band_mean = band_total / (rows * sky_count * cols)
    depth_norm = (depth_map / band_mean[:, None, None]).astype(jnp.bfloat16)
    return (coadd_image.astype(jnp.bfloat16), depth_norm)


def solution(mesh):
    in_specs = (
        P(("groups", "sky", "epoch"), "band", None, None),
        P(("groups", "sky", "epoch"), None),
        P(("groups", "sky", "epoch"), None),
        P(("groups", "sky", "epoch"), None),
        P(("groups", "sky", "epoch"), "band"),
        P(("groups", "sky", "epoch"), None, None),
        P(("groups", "sky", "epoch")),
        P("band", ("groups", "sky"), None),
        P("band", ("groups", "sky")),
    )
    out_specs = (P("band", ("groups", "sky"), "epoch"), P("band", ("groups", "sky"), "epoch"))
    return jax.shard_map(
        on_device, mesh=mesh, in_specs=in_specs, out_specs=out_specs, check_vma=False
    )
```

```python
import functools

import jax
import jax.numpy as jnp
from jax import lax
from jax.experimental import pallas as pl
from jax.experimental.pallas import tpu as pltpu
from jax.sharding import PartitionSpec as P


MARGIN = 8
CAPACITY = 2
CLIP_WIDTH = 3.0
TAPS = 6
ROW_BLOCK = 8
LANES = 128
GROUP = 8
UNROLL = 12
LAG = 4
LEFT_OVER = 32
NEAR = 4


def lanczos(distance):
    inside = jnp.abs(distance) < 3.0
    return jnp.where(inside, jnp.sinc(distance) * jnp.sinc(distance / 3.0), 0.0)


def tap_weights(fractions):
    gaps = 3.0 - jnp.arange(TAPS, dtype=jnp.float32)
    rounded = lanczos(gaps - fractions[..., None]).astype(jnp.bfloat16)
    return lax.optimization_barrier(rounded).astype(jnp.float32)


def cover(shifts, taps, index, length_in):
    total = jnp.zeros((shifts.shape[0], index.shape[0]), jnp.float32)
    for tap in range(TAPS):
        source = index[None, :] - shifts[:, None] + (tap - 3)
        inside = (source >= 0) & (source < length_in)
        total = total + jnp.where(inside, taps[:, tap][:, None], 0.0)
    return jnp.clip(total, 0.0, 1.0)


def column_kernel(ints, floats, pixels, *refs):
    step = pl.program_id(0)
    slots, bands, rows, cols = pixels.shape
    blocks = cols // LANES
    edge = 16
    turn = ints[pl.num_programs(0) * slots]
    outs, (tables, turned) = refs[:-2], refs[-2:]
    parts = len(outs)
    width = cols // parts

    @pl.when(step == 0)
    def _():
        tables[...] = jnp.zeros_like(tables)

    def gap_base(first_row, count, offset):
        k = lax.broadcasted_iota(jnp.int32, (count, LANES), 0) + first_row
        j = lax.broadcasted_iota(jnp.int32, (count, LANES), 1)
        return j - k + offset

    def one(slot, table, ring):
        at = step * slots + slot
        shift = ints[at]
        weights = [floats[at * TAPS + tap] for tap in range(TAPS)]

        def band_of(base):
            gap = base - shift
            value = jnp.zeros(base.shape, jnp.float32)
            for tap in range(TAPS):
                value = jnp.where(gap == 3 - tap, weights[tap], value)
            return value.astype(jnp.bfloat16)

        diagonal = band_of(gap_base(0, LANES, 0))
        upper = band_of(gap_base(LANES - edge, edge, LANES))
        lower = band_of(gap_base(0, edge, -LANES))
        for block in range(blocks):
            low, high = block * LANES, (block + 1) * LANES
            table[low:high, low:high] = diagonal
            if block + 1 < blocks:
                table[high - edge : high, high : high + LANES] = upper
                table[high : high + edge, low:high] = lower
        source = pixels[slot].reshape(bands * rows, cols)
        warped = jnp.dot(source, table[...], preferred_element_type=jnp.float32)
        warped = warped.astype(ring.dtype)
        for part in range(parts):
            for band in range(bands):
                piece = warped[band * rows : (band + 1) * rows, part * width : (part + 1) * width]
                ring[part, :, band * width : (band + 1) * width] = piece
        for ahead in range(parts):
            outs[ahead][slot] = ring[lax.rem(turn + ahead, parts)]

    lag = tables.shape[0]

    def several(index, carry):
        for part in range(lag):
            one(index * lag + part, tables.at[part], turned.at[part])
        return carry

    lax.fori_loop(0, slots // lag, several, 0)


def warp_columns(pixels, shifts, taps, turn, parts):
    held, bands, rows, cols = pixels.shape
    width = bands * cols // parts
    return pl.pallas_call(
        column_kernel,
        grid=(held // GROUP,),
        out_shape=[jax.ShapeDtypeStruct((held, rows, width), jnp.bfloat16)] * parts,
        in_specs=[
            pl.BlockSpec(memory_space=pltpu.SMEM),
            pl.BlockSpec(memory_space=pltpu.SMEM),
            pl.BlockSpec((GROUP, bands, rows, cols), lambda g: (g, 0, 0, 0)),
        ],
        out_specs=[pl.BlockSpec((GROUP, rows, width), lambda g: (g, 0, 0))] * parts,
        scratch_shapes=[
            pltpu.VMEM((LAG, cols, cols), jnp.bfloat16),
            pltpu.VMEM((LAG, parts, rows, width), jnp.bfloat16),
        ],
        compiler_params=pltpu.CompilerParams(dimension_semantics=("arbitrary",)),
        cost_estimate=pl.CostEstimate(
            flops=2 * held * bands * rows * cols * cols,
            bytes_accessed=4 * held * bands * rows * cols,
            transcendentals=0,
        ),
        name="columns",
    )(jnp.append(shifts, turn), taps.reshape(-1), pixels)


def clip_kernel(parts, near, col_blocks, turn, *refs):
    templates, refs = refs[:near], refs[near:]
    scalars, vectors, groups = refs[:parts], refs[parts : 2 * parts], refs[2 * parts : 3 * parts]
    out, framed, sums, planes = refs[3 * parts :]
    slots, rows, width = groups[0].shape
    owners = out.shape[0]
    bands = width // LANES
    canvas_rows = rows + 2 * MARGIN
    blocks = canvas_rows // ROW_BLOCK
    cells = vectors[0].shape[1] - LEFT_OVER
    at_taps, at_column_taps, at_scales = cells, cells + TAPS, cells + 2 * TAPS
    at_start = at_scales + 3 * bands
    cols = parts * LANES
    ends = framed.shape[0]
    framed[0:MARGIN, :] = jnp.zeros((MARGIN, width), jnp.float32)
    framed[ends - MARGIN : ends, :] = jnp.zeros((MARGIN, width), jnp.float32)

    def fill(far, carry):
        for behind in range(near):
            owner = far * near + lax.rem(turn[1] - behind + near, near)
            start = pl.multiple_of(owner * rows + MARGIN, MARGIN)
            first = pl.multiple_of(owner * rows, rows)
            framed[pl.ds(start, rows), :] = templates[behind][far].astype(jnp.float32)
            sums[pl.ds(first, rows), :] = jnp.zeros((rows, width), jnp.float32)
        return carry

    lax.fori_loop(0, owners // near, fill, 0)
    sums[ends - 2 * MARGIN : ends, :] = jnp.zeros((2 * MARGIN, width), jnp.float32)

    per_part = col_blocks // parts
    cell = lax.broadcasted_iota(jnp.int32, (cells + LEFT_OVER, LANES), 0)
    column = lax.broadcasted_iota(jnp.int32, (cells + LEFT_OVER, LANES), 1)
    col_block = jnp.zeros_like(column) + turn[0] * per_part
    for number in range(1, per_part):
        col_block += (column >= number * (LANES // per_part)).astype(jnp.int32)
    expand = jnp.concatenate(
        [
            (cell - block * col_blocks == col_block).astype(jnp.float32).astype(jnp.bfloat16)
            for block in range(blocks)
        ],
        axis=1,
    )
    lane = lax.broadcasted_iota(jnp.int32, (slots, LANES), 1) + turn[0] * LANES
    for group in range(parts):
        described = vectors[group][...]
        column = lane - described[:, at_start + 2 : at_start + 3].astype(jnp.int32)
        covered = jnp.zeros((slots, LANES), jnp.float32)
        for tap in range(TAPS):
            source = column + (tap - 3)
            inside = (source >= 0) & (source < cols)
            weight = described[:, at_column_taps + tap : at_column_taps + tap + 1]
            covered = covered + jnp.where(inside, weight, 0.0)
        covered = jnp.clip(covered, 0.0, 1.0)
        usable = jnp.dot(
            described.astype(jnp.bfloat16), expand, preferred_element_type=jnp.float32
        )
        for block in range(blocks):
            lanes = slice(block * LANES, (block + 1) * LANES)
            planes[group * slots : (group + 1) * slots, lanes] = usable[:, lanes] * covered

    i = lax.broadcasted_iota(jnp.int32, (canvas_rows, LANES), 0)
    k = lax.broadcasted_iota(jnp.int32, (canvas_rows, LANES), 1)
    base = i - MARGIN - k
    ones = jnp.ones((rows, LANES), out.dtype)

    def one(group, slot):
        columns, values = groups[group], scalars[group]
        first = pl.multiple_of(values[slot, at_start].astype(jnp.int32), ROW_BLOCK)
        gap = base - values[slot, at_start + 1].astype(jnp.int32)
        table = jnp.zeros(gap.shape, jnp.float32)
        for tap in range(TAPS):
            table = jnp.where(gap == 3 - tap, values[slot, at_taps + tap], table)
        table = table.astype(columns.dtype)[:, :rows]
        source = jnp.concatenate([columns[slot], ones], axis=1)
        warped = jnp.dot(table, source, preferred_element_type=jnp.float32)
        plane = planes[pl.ds(group * slots + slot, 1), :]
        for block in range(blocks):
            low = block * ROW_BLOCK
            where = pl.ds(first + low, ROW_BLOCK)
            row_cover = jnp.clip(warped[low : low + ROW_BLOCK, width:], 0.0, 1.0)
            weight = row_cover * plane[:, block * LANES : (block + 1) * LANES]
            for band in range(bands):
                lanes = slice(band * LANES, (band + 1) * LANES)
                scale = at_scales + 3 * band
                prior = framed[where, lanes]
                pull = (warped[low : low + ROW_BLOCK, lanes] - prior) * values[slot, scale]
                value = prior * values[slot, scale + 1] + jnp.tanh(pull) * values[slot, scale + 2]
                sums[where, lanes] += weight * value

    def several(group, index, carry):
        for part in range(UNROLL):
            one(group, index * UNROLL + part)
        return carry

    for group in range(parts):
        lax.fori_loop(0, slots // UNROLL, functools.partial(several, group), 0)

    def give(owner, carry):
        start = pl.multiple_of(owner * rows + MARGIN, MARGIN)
        out[owner] = sums[pl.ds(start, rows), :].astype(out.dtype)
        return carry

    lax.fori_loop(0, owners, give, 0)


def clip_and_sum(turn, row_blocks, col_blocks, templates, described, columns):
    parts, near = len(columns), len(templates)
    slots, rows, width = columns[0].shape
    tiles = parts * slots
    owners = near * templates[0].shape[0]
    height = owners * rows + 2 * MARGIN
    scalar = pl.BlockSpec(memory_space=pltpu.SMEM)
    vector = pl.BlockSpec(memory_space=pltpu.VMEM)
    return pl.pallas_call(
        functools.partial(clip_kernel, parts, near, col_blocks),
        out_shape=jax.ShapeDtypeStruct((owners, rows, width), jnp.bfloat16),
        in_specs=[scalar] + [vector] * near + [scalar] * parts + [vector] * (2 * parts),
        out_specs=vector,
        scratch_shapes=[
            pltpu.VMEM((height, width), jnp.float32),
            pltpu.VMEM((height, width), jnp.float32),
            pltpu.VMEM((tiles, row_blocks * LANES), jnp.float32),
        ],
        compiler_params=pltpu.CompilerParams(vmem_limit_bytes=32 * 1024 * 1024),
        cost_estimate=pl.CostEstimate(
            flops=30 * tiles * (rows + 2 * MARGIN) * width,
            bytes_accessed=2 * tiles * rows * width,
            transcendentals=tiles * (rows + 2 * MARGIN) * width,
        ),
        name="clip",
    )(turn, *templates, *described, *described, *columns)


def spread(index, block_count, block):
    which = jnp.arange(block_count, dtype=jnp.int32)[:, None] == (index // block)[None, :]
    return which.astype(jnp.float32)


def summed_on_arrival(parts, axis, groups=None):
    arrived = lax.all_to_all(
        parts, axis, split_axis=0, concat_axis=0, tiled=True, axis_index_groups=groups
    )
    return functools.reduce(jnp.add, [part.astype(jnp.float32) for part in arrived])


def sky_groups():
    count = lax.axis_size("sky")
    near = NEAR if count % NEAR == 0 else 1
    far = count // near
    near_groups = [[f * near + n for n in range(near)] for f in range(far)]
    far_groups = [[f * near + n for f in range(far)] for n in range(near)]
    return near, far, near_groups, far_groups


def sum_over_sky(parts):
    near, far, near_groups, far_groups = sky_groups()
    parts = jnp.swapaxes(parts.reshape((far, near) + parts.shape[1:]), 0, 1)
    parts = summed_on_arrival(parts, "sky", near_groups).astype(jnp.bfloat16)
    return summed_on_arrival(parts, "sky", far_groups)


def gather_over_sky(shard):
    near, far, near_groups, far_groups = sky_groups()
    copies = jnp.broadcast_to(shard[None], (far,) + shard.shape)
    shards = lax.all_to_all(
        copies, "sky", split_axis=0, concat_axis=0, tiled=True, axis_index_groups=far_groups
    )
    arrived = [shards]
    for ahead in range(1, near):
        route = [(g[i], g[(i + ahead) % near]) for g in near_groups for i in range(near)]
        arrived.append(lax.ppermute(shards, "sky", route))
    return arrived


def from_epochs(pieces):
    count = lax.axis_size("epoch")
    arrived = {0: pieces[0]}
    for ahead in sorted(range(1, count), key=lambda ahead: -min(ahead, count - ahead)):
        route = [(i, (i + ahead) % count) for i in range(count)]
        arrived[ahead] = lax.ppermute(pieces[ahead], "epoch", route)
    return [arrived[ahead] for ahead in range(count)]


def on_device(
    slot_pixels,
    slot_tile,
    slot_offset,
    slot_frac,
    slot_sigma,
    clip_mask,
    slot_count,
    template,
    prior_weight,
):
    sky_count = lax.axis_size("sky")
    epoch_count = lax.axis_size("epoch")
    epoch_position = lax.axis_index("epoch")
    held, bands, rows, cols = slot_pixels.shape
    canvas_rows = rows + 2 * MARGIN
    row_blocks, col_blocks = clip_mask.shape[1:]
    cells = row_blocks * col_blocks
    part_width = cols // epoch_count
    high = lax.Precision.HIGHEST

    template_part = lax.dynamic_slice_in_dim(
        template, epoch_position * part_width, part_width, 2
    )
    sent = jnp.swapaxes(template_part, 0, 1).reshape(rows, bands * part_width)
    templates = gather_over_sky(sent)

    target = slot_tile[:, 0]
    sigmas = slot_sigma.astype(jnp.float32)
    over = 1.0 / (sigmas * sigmas)
    scale = CLIP_WIDTH * sigmas
    scales = jnp.stack([1.0 / scale, over, scale * over], 2).reshape(held, 3 * bands)
    taps = tap_weights(slot_frac.astype(jnp.float32))
    live = (jnp.arange(held, dtype=jnp.int32) < slot_count[0]).astype(jnp.float32)
    masks = clip_mask.astype(jnp.float32) * live[:, None, None]
    described = jnp.concatenate(
        [
            masks.reshape(held, cells),
            taps[:, 0],
            taps[:, 1],
            scales,
            (target * rows).astype(jnp.float32)[:, None],
            slot_offset.astype(jnp.float32),
        ],
        1,
    )
    described = jnp.pad(described, ((0, 0), (0, cells + LEFT_OVER - described.shape[1])))

    columns = warp_columns(slot_pixels, slot_offset[:, 1], taps[:, 1], epoch_position, epoch_count)
    columns = from_epochs(columns)
    described = from_epochs([described] * epoch_count)

    row_index = jnp.arange(canvas_rows, dtype=jnp.int32) - MARGIN
    col_index = epoch_position * part_width + jnp.arange(part_width, dtype=jnp.int32)
    all_index = jnp.arange(cols, dtype=jnp.int32)
    expand = spread(col_index, col_blocks, cols // col_blocks)

    row_cover = cover(slot_offset[:, 0], taps[:, 0], row_index, rows)
    col_cover = cover(slot_offset[:, 1], taps[:, 1], all_index, cols)
    block_rows = row_cover.reshape(held, row_blocks, canvas_rows // row_blocks).sum(2)
    block_cols = col_cover.reshape(held, col_blocks, cols // col_blocks).sum(2)
    block = jnp.arange(row_blocks, dtype=jnp.int32)[None, :]
    above = (target[:, None] == 0) & (block == 0)
    below = (target[:, None] == sky_count - 1) & (block == row_blocks - 1)
    block_rows = jnp.where(above | below, 0.0, block_rows)
    tile_total = jnp.sum(masks * block_rows[:, :, None] * block_cols[:, None, :], (1, 2))
    band_part = jnp.sum(tile_total[:, None] * over, 0)
    band_part = band_part + jnp.sum(prior_weight, 1) * (cols / epoch_count)

    facts = jnp.concatenate(
        [
            masks.reshape(held, cells),
            slot_offset.astype(jnp.float32),
            slot_frac.astype(jnp.float32),
            sigmas,
        ],
        1,
    )
    earlier = (target[:, None] == target[None, :]) & (
        jnp.arange(held)[None, :] < jnp.arange(held)[:, None]
    )
    position = target * CAPACITY + jnp.sum(earlier.astype(jnp.int32), 1)
    routes = jnp.arange(sky_count * CAPACITY, dtype=jnp.int32)
    chooser = (position[None, :] == routes[:, None]).astype(jnp.float32)
    chosen = jnp.dot(chooser, facts, precision=high)
    totals = jnp.broadcast_to(band_part[None, :], (chosen.shape[0], bands))
    message = jnp.concatenate([chosen, totals], 1)
    message = jnp.pad(message, ((0, 0), (0, LANES - message.shape[1])))
    message = message.reshape(sky_count, CAPACITY, LANES)
    arrived = lax.all_to_all(message, "sky", split_axis=0, concat_axis=0, tiled=True)
    arrived = jnp.concatenate(from_epochs([arrived] * epoch_count), 0)
    band_total = jnp.sum(arrived[:, 0, cells + 4 + bands : cells + 4 + 2 * bands], 0)

    def unpack(table):
        masks = table[:, :cells].reshape(-1, row_blocks, col_blocks)
        shifts = table[:, cells : cells + 2].astype(jnp.int32)
        taps = tap_weights(table[:, cells + 2 : cells + 4])
        sigmas = table[:, cells + 4 : cells + 4 + bands]
        sigmas = jnp.where(sigmas > 0.0, sigmas, 1.0)
        return masks, shifts, taps, sigmas

    own_masks, own_shift, own_taps, own_sigmas = unpack(arrived.reshape(-1, LANES))
    own_over = 1.0 / (own_sigmas * own_sigmas)
    own_rows = cover(own_shift[:, 0], own_taps[:, 0], row_index, rows)
    own_cols = cover(own_shift[:, 1], own_taps[:, 1], col_index, cols)
    own_plane = jnp.einsum("sik,kj->isj", own_masks, expand, precision=high) * own_cols[None]
    left = own_over[:, :, None, None] * own_rows.reshape(-1, 1, row_blocks, ROW_BLOCK)
    weights = jnp.einsum("sbir,isj->birj", left, own_plane, precision=high)
    weights = weights.reshape(bands, canvas_rows, part_width)
    ring = [(i, i + 1) for i in range(sky_count - 1)]
    from_above = lax.ppermute(weights[:, canvas_rows - MARGIN :], "sky", ring)
    from_below = lax.ppermute(weights[:, :MARGIN], "sky", [(j, i) for i, j in ring])
    weight_sum = weights[:, MARGIN : MARGIN + rows]
    weight_sum = weight_sum.at[:, :MARGIN].add(from_above)
    weight_sum = weight_sum.at[:, rows - MARGIN :].add(from_below)

    turn = jnp.stack([epoch_position, lax.axis_index("sky") % len(templates)])
    partial = clip_and_sum(turn, row_blocks, col_blocks, templates, described, columns)
    flux = sum_over_sky(partial)
    flux_sum = jnp.swapaxes(flux.reshape(rows, bands, part_width), 0, 1)

    prior = prior_weight[:, :, None]
    depth_map = weight_sum + prior
    coadd_image = (flux_sum + prior * template_part.astype(jnp.float32)) / depth_map
    band_mean = band_total / (rows * sky_count * cols)
    depth_norm = (depth_map / band_mean[:, None, None]).astype(jnp.bfloat16)
    return (coadd_image.astype(jnp.bfloat16), depth_norm)


def solution(mesh):
    in_specs = (
        P(("groups", "sky", "epoch"), "band", None, None),
        P(("groups", "sky", "epoch"), None),
        P(("groups", "sky", "epoch"), None),
        P(("groups", "sky", "epoch"), None),
        P(("groups", "sky", "epoch"), "band"),
        P(("groups", "sky", "epoch"), None, None),
        P(("groups", "sky", "epoch")),
        P("band", ("groups", "sky"), None),
        P("band", ("groups", "sky")),
    )
    out_specs = (P("band", ("groups", "sky"), "epoch"), P("band", ("groups", "sky"), "epoch"))
    return jax.shard_map(
        on_device, mesh=mesh, in_specs=in_specs, out_specs=out_specs, check_vma=False
    )
```
